32 devices in a mesh: dp: 1 (over z), ctx: 32 (over y, x, core).
Axes of the slice: x: 4, y: 4, z: 1, core: 2. Of those that a mesh axis runs over, the one named last changes fastest.
The devices are a block of a 4x4x8 slice.
Arguments:
- queries: bfloat16 [1, 4096, 8, 128], P('dp', 'ctx')
- keys: bfloat16 [1, 4096, 1, 128], P('dp', 'ctx')
- values: bfloat16 [1, 4096, 1, 128], P('dp', 'ctx')
- grad_out: bfloat16 [1, 4096, 8, 128], P('dp', 'ctx')
Outputs:
- output 1: bfloat16 [1, 4096, 8, 128], P('dp', 'ctx')
- output 2: bfloat16 [1, 4096, 8, 128], P('dp', 'ctx')
- output 3: bfloat16 [1, 4096, 1, 128], P('dp', 'ctx')
- output 4: bfloat16 [1, 4096, 1, 128], P('dp', 'ctx')
All inputs are finite; a program needn't handle non-finite values.
Results may differ from the reference program's by a relative error of at most 0.0061449.
Values are sent between devices in bfloat16 or wider.
A program may use at most 768 MiB of HBM per device.

```python
import jax
import jax.numpy as jnp
from jax import lax

BATCH = 1
SEQ = 4096
HQ = 8
HEAD_DIM = 128
BLOCK = 128
NEG_BIG = -1e30


def setup_inputs(seed: int = 0, part: int = 0) -> dict:
    part_key = jax.random.fold_in(jax.random.key(seed), part)
    key_q, key_k, key_v, key_do = jax.random.split(part_key, 4)
    q_shape = (BATCH, SEQ, HQ, HEAD_DIM)
    kv_shape = (BATCH, SEQ, 1, HEAD_DIM)
    queries = 1.5 * jax.random.normal(key_q, q_shape, jnp.float32)
    keys = jax.random.normal(key_k, kv_shape, jnp.float32)
    values = jax.random.normal(key_v, kv_shape, jnp.float32)
    grad_out = jax.random.normal(key_do, q_shape, jnp.float32)
    return {"queries": queries.astype(jnp.bfloat16), "keys": keys.astype(jnp.bfloat16), "values": values.astype(jnp.bfloat16), "grad_out": grad_out.astype(jnp.bfloat16)}


def reference(queries, keys, values, grad_out):
    n_kv = keys.shape[2]
    n_grp = HQ // n_kv
    n_blocks = SEQ // BLOCK
    scale = HEAD_DIM ** -0.5
    q_lead = jnp.moveaxis(queries.reshape(BATCH, n_blocks, BLOCK, n_kv, n_grp, HEAD_DIM), 1, 0)
    do_lead = jnp.moveaxis(grad_out.reshape(BATCH, n_blocks, BLOCK, n_kv, n_grp, HEAD_DIM), 1, 0)
    k_blocks = keys.reshape(BATCH, n_blocks, BLOCK, n_kv, HEAD_DIM)
    v_blocks = values.reshape(BATCH, n_blocks, BLOCK, n_kv, HEAD_DIM)
    blk_ids = jnp.arange(n_blocks)
    stat_shape = (BATCH, n_kv, n_grp, BLOCK)

    def block_scores(q_blk, k_blk, blk_idx, key_idx):
        scores = jnp.einsum("bihgd,bjhd->bhgij", q_blk.astype(jnp.float32), k_blk.astype(jnp.float32)) * scale
        q_pos = blk_idx * BLOCK + jnp.arange(BLOCK)
        k_pos = key_idx * BLOCK + jnp.arange(BLOCK)
        return jnp.where(q_pos[:, None] >= k_pos[None, :], scores, NEG_BIG)

    def forward_block(inputs):
        q_blk, blk_idx = inputs

        def loop_body(key_idx, carry):
            m_run, l_run, acc_run = carry
            k_blk = lax.dynamic_index_in_dim(k_blocks, key_idx, 1, keepdims=False)
            v_blk = lax.dynamic_index_in_dim(v_blocks, key_idx, 1, keepdims=False)
            scores = block_scores(q_blk, k_blk, blk_idx, key_idx)
            m_new = jnp.maximum(m_run, scores.max(axis=-1))
            rescale = jnp.exp(m_run - m_new)
            weights = jnp.exp(scores - m_new[..., None])
            l_new = l_run * rescale + weights.sum(axis=-1)
            w_half = weights.astype(jnp.bfloat16).astype(jnp.float32)
            acc_new = acc_run * rescale[..., None] + jnp.einsum("bhgij,bjhd->bhgid", w_half, v_blk.astype(jnp.float32))
            return m_new, l_new, acc_new

        init_carry = (jnp.full(stat_shape, NEG_BIG, jnp.float32), jnp.zeros(stat_shape, jnp.float32), jnp.zeros(stat_shape + (HEAD_DIM,), jnp.float32))
        m_fin, l_fin, acc_fin = lax.fori_loop(0, blk_idx + 1, loop_body, init_carry)
        out_blk = jnp.transpose((acc_fin / l_fin[..., None]).astype(jnp.bfloat16), (0, 3, 1, 2, 4))
        return out_blk, m_fin + jnp.log(l_fin)

    out_lead, lse_lead = lax.map(forward_block, (q_lead, blk_ids))

    def backward_block(carry, inputs):
        dk_acc, dv_acc = carry
        q_blk, do_blk, out_blk, lse_blk, blk_idx = inputs
        q_f = q_blk.astype(jnp.float32)
        do_f = do_blk.astype(jnp.float32)
        delta_row = jnp.einsum("bihgd,bihgd->bhgi", do_f, out_blk.astype(jnp.float32))

        def loop_body(key_idx, inner):
            dq_run, dk_run, dv_run = inner
            k_blk = lax.dynamic_index_in_dim(k_blocks, key_idx, 1, keepdims=False)
            v_blk = lax.dynamic_index_in_dim(v_blocks, key_idx, 1, keepdims=False)
            scores = block_scores(q_blk, k_blk, blk_idx, key_idx)
            weights = jnp.exp(scores - lse_blk[..., None])
            w_half = weights.astype(jnp.bfloat16).astype(jnp.float32)
            dp_blk = jnp.einsum("bihgd,bjhd->bhgij", do_f, v_blk.astype(jnp.float32))
            ds_half = (weights * (dp_blk - delta_row[..., None])).astype(jnp.bfloat16).astype(jnp.float32)
            dq_run = dq_run + jnp.einsum("bhgij,bjhd->bihgd", ds_half, k_blk.astype(jnp.float32))
            dk_old = lax.dynamic_index_in_dim(dk_run, key_idx, 1, keepdims=False)
            dv_old = lax.dynamic_index_in_dim(dv_run, key_idx, 1, keepdims=False)
            dk_new = dk_old + jnp.einsum("bhgij,bihgd->bjhd", ds_half, q_f)
            dv_new = dv_old + jnp.einsum("bhgij,bihgd->bjhd", w_half, do_f)
            dk_run = lax.dynamic_update_index_in_dim(dk_run, dk_new, key_idx, 1)
            dv_run = lax.dynamic_update_index_in_dim(dv_run, dv_new, key_idx, 1)
            return dq_run, dk_run, dv_run

        dq_blk, dk_acc, dv_acc = lax.fori_loop(0, blk_idx + 1, loop_body, (jnp.zeros(q_f.shape, jnp.float32), dk_acc, dv_acc))
        return (dk_acc, dv_acc), dq_blk

    acc_zero = jnp.zeros((BATCH, n_blocks, BLOCK, n_kv, HEAD_DIM), jnp.float32)
    grads, dq_lead = lax.scan(backward_block, (acc_zero, acc_zero), (q_lead, do_lead, out_lead, lse_lead, blk_ids))
    attn_out = jnp.moveaxis(out_lead, 0, 1).reshape(BATCH, SEQ, HQ, HEAD_DIM)
    grad_q = (jnp.moveaxis(dq_lead, 0, 1) * scale).astype(jnp.bfloat16).reshape(BATCH, SEQ, HQ, HEAD_DIM)
    grad_k = (grads[0] * scale).astype(jnp.bfloat16).reshape(BATCH, SEQ, n_kv, HEAD_DIM)
    grad_v = grads[1].astype(jnp.bfloat16).reshape(BATCH, SEQ, n_kv, HEAD_DIM)
    return attn_out, grad_q, grad_k, grad_v
```

```python
import functools
import math

import jax
import jax.numpy as jnp
from jax import lax
from jax.experimental import pallas as pl
from jax.experimental.pallas import tpu as pltpu
from jax.sharding import PartitionSpec as P

NEG_BIG = -1e30
CHUNK = 256
LANES = 128


def dot_nt(a, b):
    return lax.dot_general(a, b, (((1,), (1,)), ((), ())), preferred_element_type=jnp.float32)


def dot_nn(a, b):
    return jnp.dot(a, b, preferred_element_type=jnp.float32)


def attn_kernel(n_grp, scale, q_ref, do_ref, k_ref, v_ref, o_ref, dq_ref, dkt_ref, dvt_ref,
                q_t, do_t, s_buf, m_buf, l_buf, acc_buf, d_buf):
    rows, d_head = q_ref.shape
    n_pair, width, _ = k_ref.shape
    dev = lax.axis_index("ctx")
    mine = dev // 2
    half = lax.rem(dev, 2)
    chunks = range(rows // CHUNK)
    to_log2 = scale * math.log2(math.e)

    q_t[...] = q_ref[...].astype(jnp.float32).T.astype(jnp.bfloat16)
    do_t[...] = do_ref[...].astype(jnp.float32).T.astype(jnp.bfloat16)
    m_buf[...] = jnp.full(m_buf.shape, NEG_BIG, jnp.float32)
    l_buf[...] = jnp.zeros(l_buf.shape, jnp.float32)
    acc_buf[...] = jnp.zeros(acc_buf.shape, jnp.float32)

    def score_step(pair, masked):
        k_blk = k_ref[pair]
        for c in chunks:
            part = pl.ds(c * CHUNK, CHUNK)
            s = dot_nt(q_ref[part, :], k_blk)
            if masked:
                tok = lax.broadcasted_iota(jnp.int32, s.shape, 0) // n_grp + (c * CHUNK // n_grp) + half * (width // 2)
                key = lax.broadcasted_iota(jnp.int32, s.shape, 1)
                s = jnp.where(tok >= key, s, NEG_BIG)
            s_buf[pair, part, :] = s
            m = m_buf[part, :]
            for j in range(width // LANES):
                m = jnp.maximum(m, s[:, j * LANES:(j + 1) * LANES])
            m_buf[part, :] = m

    def score_loop(pair, _):
        score_step(pair, False)
        return 0

    lax.fori_loop(0, mine, score_loop, 0)
    score_step(mine, True)

    for c in chunks:
        part = pl.ds(c * CHUNK, CHUNK)
        m = jnp.max(m_buf[part, :], axis=1, keepdims=True) * to_log2
        m_buf[part, :] = jnp.broadcast_to(m, (CHUNK, LANES))

    def value_loop(pair, _):
        v_blk = v_ref[pair]
        for c in chunks:
            part = pl.ds(c * CHUNK, CHUNK)
            m = m_buf[part, :]
            w = jnp.exp2(s_buf[pair, part, :] * to_log2 - jnp.concatenate([m] * (width // LANES), axis=1))
            s_buf[pair, part, :] = w
            l = l_buf[part, :]
            for j in range(width // LANES):
                l = l + w[:, j * LANES:(j + 1) * LANES]
            l_buf[part, :] = l
            acc_buf[part, :] += dot_nn(w.astype(jnp.bfloat16), v_blk)
        return 0

    lax.fori_loop(0, mine + 1, value_loop, 0)

    for c in chunks:
        part = pl.ds(c * CHUNK, CHUNK)
        l = jnp.sum(l_buf[part, :], axis=1, keepdims=True)
        out = (acc_buf[part, :] / l).astype(jnp.bfloat16)
        o_ref[part, :] = out
        l_buf[part, :] = jnp.broadcast_to(1.0 / l, (CHUNK, LANES))
        delta = jnp.sum(do_ref[part, :].astype(jnp.float32) * out.astype(jnp.float32), axis=1, keepdims=True)
        d_buf[part, :] = jnp.broadcast_to(delta, (CHUNK, LANES))
    acc_buf[...] = jnp.zeros(acc_buf.shape, jnp.float32)

    def grad_loop(pair, _):
        k_blk = k_ref[pair]
        v_blk = v_ref[pair]
        dv = jnp.zeros((d_head, width), jnp.float32)
        dk = jnp.zeros((d_head, width), jnp.float32)
        for c in chunks:
            part = pl.ds(c * CHUNK, CHUNK)
            inv = jnp.concatenate([l_buf[part, :]] * (width // LANES), axis=1)
            delta = jnp.concatenate([d_buf[part, :]] * (width // LANES), axis=1)
            p = s_buf[pair, part, :] * inv
            dp = dot_nt(do_ref[part, :], v_blk)
            ds = (p * (dp - delta)).astype(jnp.bfloat16)
            dv = dv + dot_nn(do_t[:, part], p.astype(jnp.bfloat16))
            dk = dk + dot_nn(q_t[:, part], ds)
            acc_buf[part, :] += dot_nn(ds, k_blk)
        dkt_ref[pair] = dk
        dvt_ref[pair] = dv
        return 0

    lax.fori_loop(0, mine + 1, grad_loop, 0)

    def zero_loop(pair, _):
        dkt_ref[pair] = jnp.zeros((d_head, width), jnp.float32)
        dvt_ref[pair] = jnp.zeros((d_head, width), jnp.float32)
        return 0

    lax.fori_loop(mine + 1, n_pair, zero_loop, 0)
    dq_ref[...] = (acc_buf[...] * scale).astype(jnp.bfloat16)


def solution(mesh):
    part_spec = P("dp", "ctx")
    n_dev = mesh.shape["ctx"]

    def local_step(queries, keys, values, grad_out):
        n_batch, c_len, n_q, d_head = queries.shape
        n_kv = keys.shape[2]
        n_grp = n_q // n_kv
        rows = c_len * n_q
        width = 2 * c_len
        n_pair = n_dev // 2
        scale = d_head ** -0.5
        q = queries.reshape(rows, d_head)
        do = grad_out.reshape(rows, d_head)
        k_all = lax.all_gather(keys.reshape(c_len, d_head), "ctx", axis=0, tiled=True).reshape(n_pair, width, d_head)
        v_all = lax.all_gather(values.reshape(c_len, d_head), "ctx", axis=0, tiled=True).reshape(n_pair, width, d_head)
        f32 = jnp.float32
        out, dq, dkt, dvt = pl.pallas_call(
            functools.partial(attn_kernel, n_grp, scale),
            out_shape=(
                jax.ShapeDtypeStruct((rows, d_head), jnp.bfloat16),
                jax.ShapeDtypeStruct((rows, d_head), jnp.bfloat16),
                jax.ShapeDtypeStruct((n_pair, d_head, width), f32),
                jax.ShapeDtypeStruct((n_pair, d_head, width), f32),
            ),
            in_specs=[pl.BlockSpec(memory_space=pltpu.VMEM)] * 4,
            out_specs=[pl.BlockSpec(memory_space=pltpu.VMEM)] * 4,
            scratch_shapes=[
                pltpu.VMEM((d_head, rows), jnp.bfloat16),
                pltpu.VMEM((d_head, rows), jnp.bfloat16),
                pltpu.VMEM((n_pair, rows, width), f32),
                pltpu.VMEM((rows, LANES), f32),
                pltpu.VMEM((rows, LANES), f32),
                pltpu.VMEM((rows, d_head), f32),
                pltpu.VMEM((rows, LANES), f32),
            ],
            compiler_params=pltpu.CompilerParams(vmem_limit_bytes=60 * 1024 * 1024),
            name="attn",
        )(q, do, k_all, v_all)
        both = jnp.stack([dkt, dvt]).reshape(2, n_pair, d_head, 2, c_len)
        both = jnp.transpose(both, (1, 3, 0, 4, 2))
        total = lax.psum_scatter(both.reshape(n_dev, 2, c_len, d_head), "ctx", scatter_dimension=0)
        attn_out = out.reshape(n_batch, c_len, n_q, d_head)
        grad_q = dq.reshape(n_batch, c_len, n_q, d_head)
        grad_k = (total[0] * scale).astype(jnp.bfloat16).reshape(n_batch, c_len, n_kv, d_head)
        grad_v = total[1].astype(jnp.bfloat16).reshape(n_batch, c_len, n_kv, d_head)
        return attn_out, grad_q, grad_k, grad_v

    return jax.shard_map(local_step, mesh=mesh, in_specs=(part_spec,) * 4, out_specs=(part_spec,) * 4, check_vma=False)
```

```python
import functools
import math

import jax
import jax.numpy as jnp
from jax import lax
from jax.experimental import pallas as pl
from jax.experimental.pallas import tpu as pltpu
from jax.sharding import PartitionSpec as P

NEG_BIG = -1e30
CHUNK = 256
LANES = 128
LAG = 2
KEY, VALUE = 0, 1
F32 = jnp.float32
BF16 = jnp.bfloat16


def dot_nt(a, b):
    return lax.dot_general(a, b, (((1,), (1,)), ((), ())), preferred_element_type=F32)


def dot_nn(a, b):
    return jnp.dot(a, b, preferred_element_type=F32)


class Tree:
    def __init__(self, side):
        self.side = side
        offsets = [(dx, dy) for dx in range(side) for dy in range(side)]
        self.order = sorted(offsets, key=lambda o: (sum(min(v, side - v) for v in o), o))
        self.slot = {o: i for i, o in enumerate(self.order)}
        self.hops = [(1, 0), (side - 1, 0), (0, 1), (0, side - 1)]

    def parent(self, tensor, off):
        side = self.side
        a, b = off if tensor == KEY else off[::-1]
        if b:
            near = b if 2 * b != side else (side - 1 if a < side // 2 else 1)
            hop = (0, 1 if 2 * near < side else side - 1)
        elif a:
            near = a if 2 * a != side else (side - 1 if tensor == KEY else 1)
            hop = (1 if 2 * near < side else side - 1, 0)
        else:
            return None
        return hop if tensor == KEY else hop[::-1]

    def children(self, tensor, off):
        side = self.side
        found = []
        for hop in self.hops:
            there = tuple((o - h) % side for o, h in zip(off, hop))
            back = tuple((-h) % side for h in hop)
            if self.parent(tensor, there) == back:
                found.append((hop, self.slot[there]))
        return found


def attn_kernel(tree, n_grp, scale, q_hbm, do_hbm, k_hbm, v_hbm, o_hbm, dq_hbm, dk_hbm, dv_hbm,
                q_s, do_s, kv_s, q_t, do_t, s_buf, m_buf, l_buf, acc_buf, d_buf, out_s, kv_out,
                part, side_in, tree_in,
                load_sem, store_sem, ag_send, ag_recv, agd_send, agd_recv, rs_send, rs_recv, rsd_send, rsd_recv):
    rows, d_head = q_s.shape
    c_len = k_hbm.shape[0]
    width = 2 * c_len
    side = tree.side
    n_slot = side * side
    dev = lax.axis_index("ctx")
    core = lax.rem(dev, 2)
    mine = dev // 2
    at_x = lax.rem(mine, side)
    at_y = mine // side
    sibling = {"ctx": mine * 2 + 1 - core}
    chunks = range(rows // CHUNK)
    to_log2 = scale * math.log2(math.e)
    own_rows = pl.ds(pl.multiple_of(core * c_len, c_len), c_len)

    def chip_at(off):
        return lax.rem(at_y + off[1], side) * side + lax.rem(at_x + off[0], side)

    def near(hop):
        return {"ctx": chip_at(hop) * 2 + core}

    loads = [
        pltpu.make_async_copy(k_hbm, kv_s.at[KEY, 0, own_rows, :], load_sem.at[0]),
        pltpu.make_async_copy(v_hbm, kv_s.at[VALUE, 0, own_rows, :], load_sem.at[1]),
        pltpu.make_async_copy(q_hbm, q_s, load_sem.at[2]),
        pltpu.make_async_copy(do_hbm, do_s, load_sem.at[3]),
    ]
    for copy in loads:
        copy.start()

    barrier = pltpu.get_barrier_semaphore()
    peers = [near(hop) for hop in tree.hops] + [sibling]
    for peer in peers:
        pl.semaphore_signal(barrier, inc=1, device_id=peer, device_id_type=pl.DeviceIdType.MESH)
    pl.semaphore_wait(barrier, len(peers))

    def remote(src, dst, send, recv, peer):
        return pltpu.make_async_remote_copy(src_ref=src, dst_ref=dst, send_sem=send, recv_sem=recv,
                                            device_id=peer, device_id_type=pl.DeviceIdType.MESH)

    def gather_copy(tensor, hop, slot, slot_there):
        return remote(kv_s.at[tensor, slot, own_rows, :], kv_s.at[tensor, slot_there, own_rows, :],
                      ag_send.at[tensor, slot_there], ag_recv.at[tensor, slot_there], near(hop))

    def gather_side(tensor, slot):
        block = kv_s.at[tensor, slot, own_rows, :]
        return remote(block, block, agd_send.at[tensor, slot], agd_recv.at[tensor, slot], sibling)

    def gather_forward(tensor, slot):
        if slot:
            gather_copy(tensor, tree.parent(tensor, tree.order[slot]), slot, slot).wait_recv()
        for hop, slot_there in tree.children(tensor, tree.order[slot]):
            gather_copy(tensor, hop, slot, slot_there).start()
        gather_side(tensor, slot).start()

    def score_step(slot):
        masked = slot == 0
        k_blk = kv_s[KEY, slot]
        for c in chunks:
            rng = pl.ds(c * CHUNK, CHUNK)
            s = dot_nt(q_s[rng, :], k_blk)
            if masked:
                tok = lax.broadcasted_iota(jnp.int32, s.shape, 0) // n_grp + (c * CHUNK // n_grp) + core * c_len
                key = lax.broadcasted_iota(jnp.int32, s.shape, 1)
                s = jnp.where(tok >= key, s, NEG_BIG)
            s_buf[slot, rng, :] = s
            m = jnp.full((CHUNK, LANES), NEG_BIG, F32) if masked else m_buf[rng, :]
            for j in range(width // LANES):
                m = jnp.maximum(m, s[:, j * LANES:(j + 1) * LANES])
            m_buf[rng, :] = m

    loads[0].wait()
    loads[1].wait()
    gather_forward(KEY, 0)
    gather_forward(VALUE, 0)
    loads[2].wait()
    loads[3].wait()
    q_t[...] = q_s[...].astype(F32).T.astype(BF16)
    do_t[...] = do_s[...].astype(F32).T.astype(BF16)
    l_buf[...] = jnp.zeros(l_buf.shape, F32)
    acc_buf[...] = jnp.zeros(acc_buf.shape, F32)

    for step in range(n_slot + 1):
        if 0 < step < n_slot:
            gather_forward(KEY, step)
            gather_forward(VALUE, step)
        if step:
            slot = step - 1
            gather_side(KEY, slot).wait_recv()
            pl.when(chip_at(tree.order[slot]) <= mine)(functools.partial(score_step, slot))
    for slot in range(n_slot):
        gather_side(VALUE, slot).wait_recv()

    for c in chunks:
        rng = pl.ds(c * CHUNK, CHUNK)
        m = jnp.max(m_buf[rng, :], axis=1, keepdims=True) * to_log2
        m_buf[rng, :] = jnp.broadcast_to(m, (CHUNK, LANES))

    xs = sum(o[0] << (2 * i) for i, o in enumerate(tree.order))
    ys = sum(o[1] << (2 * i) for i, o in enumerate(tree.order))

    def slot_chip(slot):
        def field(packed):
            signed = packed - (1 << 32) if packed >= 1 << 31 else packed
            return lax.shift_right_logical(jnp.int32(signed), 2 * slot) & 3
        return chip_at((field(xs), field(ys)))

    def value_step(slot):
        v_blk = kv_s[VALUE, slot]
        for c in chunks:
            rng = pl.ds(c * CHUNK, CHUNK)
            m = m_buf[rng, :]
            w = jnp.exp2(s_buf[slot, rng, :] * to_log2 - jnp.concatenate([m] * (width // LANES), axis=1))
            s_buf[slot, rng, :] = w
            l = l_buf[rng, :]
            for j in range(width // LANES):
                l = l + w[:, j * LANES:(j + 1) * LANES]
            l_buf[rng, :] = l
            acc_buf[rng, :] += dot_nn(w.astype(BF16), v_blk)

    @pl.loop(0, n_slot)
    def _(slot):
        pl.when(slot_chip(slot) <= mine)(lambda: value_step(slot))

    for c in chunks:
        rng = pl.ds(c * CHUNK, CHUNK)
        l = jnp.sum(l_buf[rng, :], axis=1, keepdims=True)
        out = (acc_buf[rng, :] / l).astype(BF16)
        out_s[0, rng, :] = out
        l_buf[rng, :] = jnp.broadcast_to(1.0 / l, (CHUNK, LANES))
        delta = jnp.sum(do_s[rng, :].astype(F32) * out.astype(F32), axis=1, keepdims=True)
        d_buf[rng, :] = jnp.broadcast_to(delta, (CHUNK, LANES))
    store_o = pltpu.make_async_copy(out_s.at[0], o_hbm, store_sem.at[0])
    store_o.start()
    acc_buf[...] = jnp.zeros(acc_buf.shape, F32)

    def side_copy(tensor, slot):
        return remote(part.at[tensor, slot, 1 - core], side_in.at[tensor, slot],
                      rsd_send.at[tensor, slot], rsd_recv.at[tensor, slot], sibling)

    def tree_copy(tensor, slot):
        hop = tree.parent(tensor, tree.order[slot])
        return remote(part.at[tensor, slot, core], tree_in.at[tensor, slot],
                      rs_send.at[tensor, slot], rs_recv.at[tensor, slot], near(hop))

    def grad_step(slot):
        k_blk = kv_s[KEY, slot]
        v_blk = kv_s[VALUE, slot]
        dv = jnp.zeros((d_head, width), F32)
        dk = jnp.zeros((d_head, width), F32)
        for c in chunks:
            rng = pl.ds(c * CHUNK, CHUNK)
            inv = jnp.concatenate([l_buf[rng, :]] * (width // LANES), axis=1)
            delta = jnp.concatenate([d_buf[rng, :]] * (width // LANES), axis=1)
            p = s_buf[slot, rng, :] * inv
            dp = dot_nt(do_s[rng, :], v_blk)
            ds = (p * (dp - delta)).astype(BF16)
            dv = dv + dot_nn(do_t[:, rng], p.astype(BF16))
            dk = dk + dot_nn(q_t[:, rng], ds)
            acc_buf[rng, :] += dot_nn(ds, k_blk)
        for h in range(2):
            part[KEY, slot, h] = dk[:, h * c_len:(h + 1) * c_len]
            part[VALUE, slot, h] = dv[:, h * c_len:(h + 1) * c_len]

    def zero_step(slot):
        part[:, slot] = jnp.zeros(part.shape[:1] + part.shape[2:], F32)

    def merge(slot):
        for tensor in (KEY, VALUE):
            side_copy(tensor, slot).wait_recv()
            total = part[tensor, slot, core] + side_in[tensor, slot]
            for _, child in tree.children(tensor, tree.order[slot]):
                tree_copy(tensor, child).wait_recv()
                total = total + tree_in[tensor, child]
            if slot:
                part[tensor, slot, core] = total
                tree_copy(tensor, slot).start()
            else:
                total = total * scale if tensor == KEY else total
                kv_out[tensor] = total.T.astype(BF16)

    @pl.loop(0, n_slot)
    def _(step):
        slot = n_slot - 1 - step
        active = slot_chip(slot) <= mine
        pl.when(active)(lambda: grad_step(slot))
        pl.when(jnp.logical_not(active))(lambda: zero_step(slot))
        for tensor in (KEY, VALUE):
            side_copy_dyn = remote(part.at[tensor, slot, 1 - core], side_in.at[tensor, slot],
                                   rsd_send.at[tensor, slot], rsd_recv.at[tensor, slot], sibling)
            side_copy_dyn.start()
        for s in range(LAG, n_slot):
            pl.when(slot == s - LAG)(functools.partial(merge, s))

    for c in chunks:
        rng = pl.ds(c * CHUNK, CHUNK)
        out_s[1, rng, :] = (acc_buf[rng, :] * scale).astype(BF16)
    store_dq = pltpu.make_async_copy(out_s.at[1], dq_hbm, store_sem.at[1])
    store_dq.start()
    for s in reversed(range(LAG)):
        merge(s)
    store_dk = pltpu.make_async_copy(kv_out.at[KEY], dk_hbm, store_sem.at[2])
    store_dv = pltpu.make_async_copy(kv_out.at[VALUE], dv_hbm, store_sem.at[3])
    store_dk.start()
    store_dv.start()

    for tensor in (KEY, VALUE):
        for slot in range(n_slot):
            gather_side(tensor, slot).wait_send()
            side_copy(tensor, slot).wait_send()
            for hop, slot_there in tree.children(tensor, tree.order[slot]):
                gather_copy(tensor, hop, slot, slot_there).wait_send()
            if slot:
                tree_copy(tensor, slot).wait_send()
    for copy in (store_o, store_dq, store_dk, store_dv):
        copy.wait()


def solution(mesh):
    part_spec = P("dp", "ctx")
    n_dev = mesh.shape["ctx"]
    tree = Tree(math.isqrt(n_dev // 2))

    def local_step(queries, keys, values, grad_out):
        n_batch, c_len, n_q, d_head = queries.shape
        n_kv = keys.shape[2]
        n_grp = n_q // n_kv
        rows = c_len * n_q
        width = 2 * c_len
        n_slot = n_dev // 2
        scale = d_head ** -0.5
        blocks = (2, n_slot)
        any_spec = pl.BlockSpec(memory_space=pl.ANY)
        out, dq, dk, dv = pl.pallas_call(
            functools.partial(attn_kernel, tree, n_grp, scale),
            out_shape=(
                jax.ShapeDtypeStruct((rows, d_head), BF16),
                jax.ShapeDtypeStruct((rows, d_head), BF16),
                jax.ShapeDtypeStruct((c_len, d_head), BF16),
                jax.ShapeDtypeStruct((c_len, d_head), BF16),
            ),
            in_specs=[any_spec] * 4,
            out_specs=[any_spec] * 4,
            scratch_shapes=[
                pltpu.VMEM((rows, d_head), BF16),
                pltpu.VMEM((rows, d_head), BF16),
                pltpu.VMEM(blocks + (width, d_head), BF16),
                pltpu.VMEM((d_head, rows), BF16),
                pltpu.VMEM((d_head, rows), BF16),
                pltpu.VMEM((n_slot, rows, width), F32),
                pltpu.VMEM((rows, LANES), F32),
                pltpu.VMEM((rows, LANES), F32),
                pltpu.VMEM((rows, d_head), F32),
                pltpu.VMEM((rows, LANES), F32),
                pltpu.VMEM((2, rows, d_head), BF16),
                pltpu.VMEM((2, c_len, d_head), BF16),
                pltpu.VMEM(blocks + (2, d_head, c_len), F32),
                pltpu.VMEM(blocks + (d_head, c_len), F32),
                pltpu.VMEM(blocks + (d_head, c_len), F32),
                pltpu.SemaphoreType.DMA((4,)),
                pltpu.SemaphoreType.DMA((4,)),
            ] + [pltpu.SemaphoreType.DMA(blocks)] * 8,
            compiler_params=pltpu.CompilerParams(
                vmem_limit_bytes=60 * 1024 * 1024, collective_id=0, has_side_effects=True),
            name="attn",
        )(queries.reshape(rows, d_head), grad_out.reshape(rows, d_head),
          keys.reshape(c_len, d_head), values.reshape(c_len, d_head))
        q_shape = (n_batch, c_len, n_q, d_head)
        kv_shape = (n_batch, c_len, n_kv, d_head)
        return out.reshape(q_shape), dq.reshape(q_shape), dk.reshape(kv_shape), dv.reshape(kv_shape)

    return jax.shard_map(local_step, mesh=mesh, in_specs=(part_spec,) * 4, out_specs=(part_spec,) * 4, check_vma=False)
```

```python
import functools
import math

import jax
import jax.numpy as jnp
from jax import lax
from jax.experimental import pallas as pl
from jax.experimental.pallas import tpu as pltpu
from jax.sharding import PartitionSpec as P

NEG_BIG = -1e30
CHUNK = 256
LANES = 128
LAG = 2
QUERIES = {11: 1, 9: 1, 4: 2}
KEY, VALUE = 0, 1
F32 = jnp.float32
BF16 = jnp.bfloat16


def dot_nt(a, b):
    return lax.dot_general(a, b, (((1,), (1,)), ((), ())), preferred_element_type=F32)


def dot_nn(a, b):
    return jnp.dot(a, b, preferred_element_type=F32)


class Tree:
    def __init__(self, side):
        self.side = side
        offsets = [(dx, dy) for dx in range(side) for dy in range(side)]
        length = lambda v: min(v, side - v)
        self.order = sorted(offsets, key=lambda o: (length(o[0]) + length(o[1]), length(o[0]) == 2 or length(o[1]) == 2, o))
        self.slot = {o: i for i, o in enumerate(self.order)}
        self.n_near = sum(length(o[0]) < 2 and length(o[1]) < 2 for o in offsets)
        self.hops = [(1, 0), (side - 1, 0), (0, 1), (0, side - 1)]

    def parent(self, tensor, off):
        side = self.side
        a, b = off if tensor == KEY else off[::-1]
        if b:
            near = b if 2 * b != side else (side - 1 if a < side // 2 else 1)
            hop = (0, 1 if 2 * near < side else side - 1)
        elif a:
            near = a if 2 * a != side else (side - 1 if tensor == KEY else 1)
            hop = (1 if 2 * near < side else side - 1, 0)
        else:
            return None
        return hop if tensor == KEY else hop[::-1]

    def children(self, tensor, off):
        found = []
        for hop in self.hops:
            there = tuple((o - h) % self.side for o, h in zip(off, hop))
            back = tuple((-h) % self.side for h in hop)
            if there != (0, 0) and self.parent(tensor, there) == back:
                found.append(self.slot[there])
        return found

    def source(self, off):
        side = self.side
        mid, one, far = side // 2, 1, side - 1
        if mid not in off:
            return off
        if off == (mid, mid):
            return (one, one)
        if off[0] == mid:
            return (one if off[1] == 0 else far, 0)
        return (0, one if off[0] == 0 else far)

    def targets(self, slot):
        found = []
        for there in range(1, len(self.order)):
            src = self.source(self.order[there])
            if tuple((o - e) % self.side for o, e in zip(self.order[there], src)) == self.order[slot]:
                found.append((tuple((-e) % self.side for e in src), there))
        return found


    def takers(self, slot):
        found = [(0, 0)]
        for off, there in self.targets(slot):
            found += [self.move(off, o) for o in self.takers(there)]
        return found

    def givers(self, tensor, slot):
        found = [(0, 0)]
        for child in self.children(tensor, self.order[slot]):
            hop = self.hop_to(slot, child)
            found += [self.move(hop, o) for o in self.givers(tensor, child)]
        return found

    def move(self, a, b):
        return tuple((i + j) % self.side for i, j in zip(a, b))

    def hop_to(self, slot, child):
        return tuple((i - j) % self.side for i, j in zip(self.order[slot], self.order[child]))


def attn_kernel(tree, n_grp, scale, q_hbm, do_hbm, k_hbm, v_hbm, o_hbm, dq_hbm, dk_hbm, dv_hbm,
                q_s, do_s, kv_s, q_t, do_t, s_buf, dp_buf, ds_buf, m_buf, top_buf, l_buf, acc_buf, d_buf, out_s, kv_out,
                part, side_in, tree_in, local_sem, gather_sem, cross_sem, side_sem, tree_sem, sent_sem):
    rows, d_head = q_s.shape
    c_len = k_hbm.shape[0]
    width = 2 * c_len
    side = tree.side
    n_slot = side * side
    n_near = tree.n_near
    dev = lax.axis_index("ctx")
    core = lax.rem(dev, 2)
    mine = dev // 2
    at_x = lax.rem(mine, side)
    at_y = mine // side
    sibling = {"ctx": mine * 2 + 1 - core}
    chunks = [pl.ds(i * CHUNK, CHUNK) for i in range(rows // CHUNK)]
    to_log2 = scale * math.log2(math.e)
    own_rows = pl.ds(pl.multiple_of(core * c_len, c_len), c_len)

    def chip_at(off):
        return lax.rem(at_y + off[1], side) * side + lax.rem(at_x + off[0], side)

    def near(off):
        return {"ctx": chip_at(off) * 2 + core}

    def wide(x):
        return jnp.concatenate([x] * (width // LANES), axis=1)

    loads = [
        pltpu.make_async_copy(k_hbm, kv_s.at[0, KEY, own_rows, :], local_sem.at[0]),
        pltpu.make_async_copy(v_hbm, kv_s.at[0, VALUE, own_rows, :], local_sem.at[1]),
        pltpu.make_async_copy(q_hbm, q_s, local_sem.at[2]),
        pltpu.make_async_copy(do_hbm, do_s, local_sem.at[3]),
    ]
    for copy in loads:
        copy.start()

    with jax.named_scope("barrier"):
        barrier = pltpu.get_barrier_semaphore()
        peers = [near(off) for off in tree.order[1:n_near]] + [sibling]
        for peer in peers:
            pl.semaphore_signal(barrier, inc=1, device_id=peer, device_id_type=pl.DeviceIdType.MESH)
        pl.semaphore_wait(barrier, len(peers))

    def remote(src, dst, send, recv, peer):
        return pltpu.make_async_remote_copy(src_ref=src, dst_ref=dst, send_sem=send, recv_sem=recv,
                                            device_id=peer, device_id_type=pl.DeviceIdType.MESH)

    def gather_copy(slot, off, there):
        return remote(kv_s.at[slot, :, own_rows, :], kv_s.at[there, :, own_rows, :],
                      sent_sem.at[0, there], gather_sem.at[there], near(off))

    def cross_copy(slot):
        block = kv_s.at[slot, :, own_rows, :]
        return remote(block, block, sent_sem.at[1, slot], cross_sem.at[slot], sibling)

    def side_copy(slot):
        return remote(part.at[slot, 1 - core], side_in.at[slot], sent_sem.at[1, slot], side_sem.at[slot], sibling)

    def tree_copy(tensor, slot):
        hop = tree.parent(tensor, tree.order[slot])
        return remote(part.at[slot, core, tensor], tree_in.at[tensor, slot],
                      sent_sem.at[2 * tensor, slot], tree_sem.at[tensor, slot], near(hop))

    def concerns(slot, offsets):
        owner = chip_at(tree.order[slot])
        return functools.reduce(jnp.logical_or, [chip_at(o) >= owner for o in offsets])

    def taken(slot, off, there):
        return concerns(slot, [tree.move(off, o) for o in tree.takers(there)])

    def given(tensor, slot, child):
        return concerns(slot, [tree.move(tree.hop_to(slot, child), o) for o in tree.givers(tensor, child)])

    def active(slot):
        return slot_chip(slot) <= mine

    def each_target(slot, act):
        for off, there in tree.targets(slot):
            pl.when(taken(slot, off, there))(functools.partial(act, slot, off, there))

    def arrive(first, last):
        for slot in range(first, last):
            if slot:
                pl.when(concerns(slot, tree.takers(slot)))(
                    gather_copy(slot, tree.source(tree.order[slot]), slot).wait_recv)
            each_target(slot, lambda *which: gather_copy(*which).start())
            pl.when(active(slot))(cross_copy(slot).start)

    xs = sum(o[0] << (2 * i) for i, o in enumerate(tree.order))
    ys = sum(o[1] << (2 * i) for i, o in enumerate(tree.order))

    def slot_chip(slot):
        def field(packed):
            signed = packed - (1 << 32) if packed >= 1 << 31 else packed
            return lax.shift_right_logical(jnp.int32(signed), 2 * slot) & 3
        return chip_at((field(xs), field(ys)))

    def score_step(slot, masked):
        k_blk = kv_s[slot, KEY]
        v_blk = kv_s[slot, VALUE]
        for c, rng in enumerate(chunks):
            s = dot_nt(q_s[rng, :], k_blk)
            if masked:
                tok = lax.broadcasted_iota(jnp.int32, s.shape, 0) // n_grp + (c * CHUNK // n_grp) + core * c_len
                key = lax.broadcasted_iota(jnp.int32, s.shape, 1)
                s = jnp.where(tok >= key, s, NEG_BIG)
            s_buf[slot, rng, :] = s
            m = jnp.full((CHUNK, LANES), NEG_BIG, F32) if masked else m_buf[rng, :]
            for j in range(width // LANES):
                m = jnp.maximum(m, s[:, j * LANES:(j + 1) * LANES])
            m_buf[rng, :] = m
            dp_buf[slot, rng, :] = dot_nt(do_s[rng, :], v_blk)

    def value_step(slot):
        v_blk = kv_s[slot, VALUE]
        for rng in chunks:
            w = jnp.exp2(s_buf[slot, rng, :] * to_log2 - wide(top_buf[rng, :]))
            l = l_buf[rng, :]
            for j in range(width // LANES):
                l = l + w[:, j * LANES:(j + 1) * LANES]
            l_buf[rng, :] = l
            acc_buf[rng, :] += dot_nn(w.astype(BF16), v_blk)

    def top_step(again):
        for rng in chunks:
            top = jnp.max(m_buf[rng, :], axis=1, keepdims=True) * to_log2
            top = jnp.broadcast_to(top, (CHUNK, LANES))
            if again:
                shrink = jnp.exp2(top_buf[rng, :] - top)
                l_buf[rng, :] = l_buf[rng, :] * shrink
                acc_buf[rng, :] = acc_buf[rng, :] * shrink
            top_buf[rng, :] = top

    def score_loop(first, last):
        @pl.loop(first, last)
        def _(slot):
            @pl.when(active(slot))
            def _():
                cross_copy(slot).wait_recv()
                score_step(slot, False)

    def value_loop(first, last):
        @pl.loop(first, last)
        def _(slot):
            @pl.when(active(slot))
            def _():
                value_step(slot)
                cross_copy(slot).wait_send()

    loads[0].wait()
    loads[1].wait()
    arrive(0, 1)
    loads[2].wait()
    loads[3].wait()
    with jax.named_scope("first"):
        q_t[...] = q_s[...].astype(F32).T.astype(BF16)
        do_t[...] = do_s[...].astype(F32).T.astype(BF16)
        l_buf[...] = jnp.zeros(l_buf.shape, F32)
        acc_buf[...] = jnp.zeros(acc_buf.shape, F32)
        cross_copy(0).wait_recv()
        score_step(0, True)

    n_next = len(tree.hops) + 1
    with jax.named_scope("arrive_next"):
        arrive(1, n_next)
    with jax.named_scope("score_next"):
        score_loop(1, n_next)
    with jax.named_scope("arrive_near"):
        arrive(n_next, n_near)
    with jax.named_scope("score_near"):
        score_loop(n_next, n_near)
    with jax.named_scope("value_near"):
        top_step(False)
        value_loop(0, n_near)
    with jax.named_scope("arrive_far"):
        arrive(n_near, n_slot)
    with jax.named_scope("score_far"):
        score_loop(n_near, n_slot)
    with jax.named_scope("value_far"):
        top_step(True)
        value_loop(n_near, n_slot)

    with jax.named_scope("out"):
        for rng in chunks:
            l = jnp.sum(l_buf[rng, :], axis=1, keepdims=True)
            out = (acc_buf[rng, :] / l).astype(BF16)
            out_s[0, rng, :] = out
            top_buf[rng, :] = top_buf[rng, :] + jnp.broadcast_to(jnp.log2(l), (CHUNK, LANES))
            delta = jnp.sum(do_s[rng, :].astype(F32) * out.astype(F32), axis=1, keepdims=True)
            d_buf[rng, :] = jnp.broadcast_to(delta, (CHUNK, LANES))
        store_o = pltpu.make_async_copy(out_s.at[0], o_hbm, local_sem.at[0])
        store_o.start()
        acc_buf[...] = jnp.zeros(acc_buf.shape, F32)
        for slot in range(n_near):
            each_target(slot, lambda *which: gather_copy(*which).wait_send())

    def grad_step(slot):
        dv = jnp.zeros((d_head, width), F32)
        dk = jnp.zeros((d_head, width), F32)
        for rng in chunks:
            p = jnp.exp2(s_buf[slot, rng, :] * to_log2 - wide(top_buf[rng, :]))
            ds = (p * (dp_buf[slot, rng, :] - wide(d_buf[rng, :]))).astype(BF16)
            ds_buf[slot, rng, :] = ds
            dv = dv + dot_nn(do_t[:, rng], p.astype(BF16))
            dk = dk + dot_nn(q_t[:, rng], ds)
        for h in range(2):
            part[slot, h, KEY] = dk[:, h * c_len:(h + 1) * c_len]
            part[slot, h, VALUE] = dv[:, h * c_len:(h + 1) * c_len]

    def zero_step(slot):
        part[slot] = jnp.zeros(part.shape[1:], F32)

    def merge(slot):
        @pl.when(active(slot))
        def _():
            side_copy(slot).wait_recv()
            part[slot, core] = part[slot, core] + side_in[slot]

        for tensor in (KEY, VALUE):
            for child in tree.children(tensor, tree.order[slot]):
                @pl.when(given(tensor, slot, child))
                def _():
                    tree_copy(tensor, child).wait_recv()
                    part[slot, core, tensor] = part[slot, core, tensor] + tree_in[tensor, child]
            if slot:
                pl.when(concerns(slot, tree.givers(tensor, slot)))(tree_copy(tensor, slot).start)
        if slot == 0:
            kv_out[KEY] = (part[0, core, KEY] * scale).T.astype(BF16)
            kv_out[VALUE] = part[0, core, VALUE].T.astype(BF16)

    def sums_sent(first, last):
        for slot in range(first, last):
            for tensor in (KEY, VALUE):
                pl.when(concerns(slot, tree.givers(tensor, slot)))(tree_copy(tensor, slot).wait_send)

    def query_step(slot):
        k_blk = kv_s[slot, KEY]
        for rng in chunks:
            acc_buf[rng, :] += dot_nn(ds_buf[slot, rng, :], k_blk)

    def query_loop(first, last):
        if first < last:
            with jax.named_scope(f"query#n={last - first}"):
                @pl.loop(first, last)
                def _(slot):
                    pl.when(active(slot))(lambda: query_step(slot))

    left = n_slot
    before = {}
    for slot in reversed(range(n_slot)):
        taken = min(QUERIES.get(slot, 0), left)
        before[slot] = (left - taken, left)
        left -= taken

    def merge_after_queries(slot):
        query_loop(*before[slot])
        with jax.named_scope(f"merge#s={slot}"):
            merge(slot)

    @pl.loop(0, n_slot)
    def _(step):
        slot = n_slot - 1 - step

        @pl.when(active(slot))
        def _():
            with jax.named_scope("grad"):
                grad_step(slot)
            side_copy(slot).start()

        pl.when(jnp.logical_not(active(slot)))(lambda: zero_step(slot))
        for s in range(LAG, n_slot):
            pl.when(slot == s - LAG)(functools.partial(merge_after_queries, s))

    for s in reversed(range(1, LAG)):
        merge_after_queries(s)
    query_loop(0, left)
    with jax.named_scope("query_out"):
        for rng in chunks:
            out_s[1, rng, :] = (acc_buf[rng, :] * scale).astype(BF16)
        store_dq = pltpu.make_async_copy(out_s.at[1], dq_hbm, local_sem.at[1])
        store_dq.start()
    with jax.named_scope("drain"):
        sums_sent(len(tree.hops) + 1, n_slot)

        @pl.loop(0, n_slot)
        def _(slot):
            pl.when(active(slot))(lambda: side_copy(slot).wait_send())

    with jax.named_scope("merge#s=0"):
        merge(0)
    store_dk = pltpu.make_async_copy(kv_out.at[KEY], dk_hbm, local_sem.at[2])
    store_dv = pltpu.make_async_copy(kv_out.at[VALUE], dv_hbm, local_sem.at[3])
    store_dk.start()
    store_dv.start()
    sums_sent(1, len(tree.hops) + 1)
    with jax.named_scope("store"):
        for copy in (store_o, store_dq, store_dk, store_dv):
            copy.wait()


def solution(mesh):
    part_spec = P("dp", "ctx")
    n_dev = mesh.shape["ctx"]
    tree = Tree(math.isqrt(n_dev // 2))

    def local_step(queries, keys, values, grad_out):
        n_batch, c_len, n_q, d_head = queries.shape
        n_kv = keys.shape[2]
        n_grp = n_q // n_kv
        rows = c_len * n_q
        width = 2 * c_len
        n_slot = n_dev // 2
        scale = d_head ** -0.5
        any_spec = pl.BlockSpec(memory_space=pl.ANY)
        dma_sem = pltpu.SemaphoreType.DMA
        out, dq, dk, dv = pl.pallas_call(
            functools.partial(attn_kernel, tree, n_grp, scale),
            out_shape=(
                jax.ShapeDtypeStruct((rows, d_head), BF16),
                jax.ShapeDtypeStruct((rows, d_head), BF16),
                jax.ShapeDtypeStruct((c_len, d_head), BF16),
                jax.ShapeDtypeStruct((c_len, d_head), BF16),
            ),
            in_specs=[any_spec] * 4,
            out_specs=[any_spec] * 4,
            scratch_shapes=[
                pltpu.VMEM((rows, d_head), BF16),
                pltpu.VMEM((rows, d_head), BF16),
                pltpu.VMEM((n_slot, 2, width, d_head), BF16),
                pltpu.VMEM((d_head, rows), BF16),
                pltpu.VMEM((d_head, rows), BF16),
                pltpu.VMEM((n_slot, rows, width), F32),
                pltpu.VMEM((n_slot, rows, width), F32),
                pltpu.VMEM((n_slot, rows, width), BF16),
                pltpu.VMEM((rows, LANES), F32),
                pltpu.VMEM((rows, LANES), F32),
                pltpu.VMEM((rows, LANES), F32),
                pltpu.VMEM((rows, d_head), F32),
                pltpu.VMEM((rows, LANES), F32),
                pltpu.VMEM((2, rows, d_head), BF16),
                pltpu.VMEM((2, c_len, d_head), BF16),
                pltpu.VMEM((n_slot, 2, 2, d_head, c_len), F32),
                pltpu.VMEM((n_slot, 2, d_head, c_len), F32),
                pltpu.VMEM((2, n_slot, d_head, c_len), F32),
                dma_sem((4,)),
                dma_sem((n_slot,)),
                dma_sem((n_slot,)),
                dma_sem((n_slot,)),
                dma_sem((2, n_slot)),
                dma_sem((3, n_slot)),
            ],
            compiler_params=pltpu.CompilerParams(
                vmem_limit_bytes=60 * 1024 * 1024, collective_id=0, has_side_effects=True),
            name="attn",
        )(queries.reshape(rows, d_head), grad_out.reshape(rows, d_head),
          keys.reshape(c_len, d_head), values.reshape(c_len, d_head))
        q_shape = (n_batch, c_len, n_q, d_head)
        kv_shape = (n_batch, c_len, n_kv, d_head)
        return out.reshape(q_shape), dq.reshape(q_shape), dk.reshape(kv_shape), dv.reshape(kv_shape)

    return jax.shard_map(local_step, mesh=mesh, in_specs=(part_spec,) * 4, out_specs=(part_spec,) * 4, check_vma=False)
```

```python
import functools
import math

import jax
import jax.numpy as jnp
from jax import lax
from jax.experimental import pallas as pl
from jax.experimental.pallas import tpu as pltpu
from jax.sharding import PartitionSpec as P

NEG_BIG = -1e30
CHUNK = 256
SUBLANES = 8
LAG = 2
QUERIES = {}
KEY, VALUE = 0, 1
F32 = jnp.float32
BF16 = jnp.bfloat16


def dot_tn(a, b):
    return lax.dot_general(a, b, (((0,), (0,)), ((), ())), preferred_element_type=F32)


def dot_nn(a, b):
    return jnp.dot(a, b, preferred_element_type=F32)


def fold(x):
    return x.reshape(x.shape[0] // SUBLANES, SUBLANES, x.shape[1])


def spread(x):
    return jnp.broadcast_to(x, (SUBLANES, x.shape[1]))


class Tree:
    def __init__(self, side):
        self.side = side
        offsets = [(dx, dy) for dx in range(side) for dy in range(side)]
        length = lambda v: min(v, side - v)
        self.order = sorted(offsets, key=lambda o: (length(o[0]) + length(o[1]), length(o[0]) == 2 or length(o[1]) == 2, o))
        self.slot = {o: i for i, o in enumerate(self.order)}
        self.n_near = sum(length(o[0]) < 2 and length(o[1]) < 2 for o in offsets)
        self.hops = [(1, 0), (side - 1, 0), (0, 1), (0, side - 1)]

    def parent(self, tensor, off):
        side = self.side
        mid, one, far = side // 2, 1, side - 1
        first, last = (one, far) if tensor == KEY else (far, one)
        if off == (0, 0):
            return None
        if off == (mid, mid):
            return (first, first)
        if off[0] == mid:
            return (first if off[1] in (0, one) else last, 0)
        if off[1] == mid:
            return (0, last if off[0] in (0, far) else first)
        if 0 in off:
            return off
        return (0, off[1]) if tensor == KEY else (off[0], 0)

    def children(self, tensor, off):
        return [there for there in range(1, len(self.order)) if off == tuple(
            (o - p) % self.side for o, p in zip(self.order[there], self.parent(tensor, self.order[there])))]

    def source(self, off):
        side = self.side
        mid, one, far = side // 2, 1, side - 1
        if mid not in off:
            return off
        if off == (mid, mid):
            return (one, one)
        if off[0] == mid:
            return (one if off[1] == 0 else far, 0)
        return (0, one if off[0] == 0 else far)

    def targets(self, slot):
        found = []
        for there in range(1, len(self.order)):
            src = self.source(self.order[there])
            if tuple((o - e) % self.side for o, e in zip(self.order[there], src)) == self.order[slot]:
                found.append((tuple((-e) % self.side for e in src), there))
        return found


    def takers(self, slot):
        found = [(0, 0)]
        for off, there in self.targets(slot):
            found += [self.move(off, o) for o in self.takers(there)]
        return found

    def givers(self, tensor, slot):
        found = [(0, 0)]
        for child in self.children(tensor, self.order[slot]):
            hop = self.hop_to(slot, child)
            found += [self.move(hop, o) for o in self.givers(tensor, child)]
        return found

    def move(self, a, b):
        return tuple((i + j) % self.side for i, j in zip(a, b))

    def hop_to(self, slot, child):
        return tuple((i - j) % self.side for i, j in zip(self.order[slot], self.order[child]))


def attn_kernel(tree, n_grp, scale, q_hbm, do_hbm, k_hbm, v_hbm, o_out, dq_out, dk_out, dv_out,
                q_s, do_s, kv_s, q_t, do_t, s_buf, dp_buf, ds_buf, m_buf, top_buf, l_buf, acc_buf, d_buf,
                part, side_in, tree_in, local_sem, gather_sem, cross_sem, side_sem, tree_sem, sent_sem):
    rows, d_head = q_s.shape
    c_len = k_hbm.shape[0]
    width = 2 * c_len
    side = tree.side
    n_slot = side * side
    n_near = tree.n_near
    dev = lax.axis_index("ctx")
    core = lax.rem(dev, 2)
    mine = dev // 2
    at_x = lax.rem(mine, side)
    at_y = mine // side
    sibling = {"ctx": mine * 2 + 1 - core}
    chunks = [pl.ds(i * CHUNK, CHUNK) for i in range(rows // CHUNK)]
    to_log2 = scale * math.log2(math.e)
    own_rows = pl.ds(pl.multiple_of(core * c_len, c_len), c_len)

    def chip_at(off):
        return lax.rem(at_y + off[1], side) * side + lax.rem(at_x + off[0], side)

    def near(off):
        return {"ctx": chip_at(off) * 2 + core}

    loads = [
        pltpu.make_async_copy(k_hbm, kv_s.at[0, KEY, own_rows, :], local_sem.at[0]),
        pltpu.make_async_copy(v_hbm, kv_s.at[0, VALUE, own_rows, :], local_sem.at[1]),
        pltpu.make_async_copy(q_hbm, q_s, local_sem.at[2]),
        pltpu.make_async_copy(do_hbm, do_s, local_sem.at[3]),
    ]
    for copy in loads:
        copy.start()

    with jax.named_scope("barrier"):
        barrier = pltpu.get_barrier_semaphore()
        peers = [near(off) for off in tree.order[1:n_near]] + [sibling]
        for peer in peers:
            pl.semaphore_signal(barrier, inc=1, device_id=peer, device_id_type=pl.DeviceIdType.MESH)
        pl.semaphore_wait(barrier, len(peers))

    def remote(src, dst, send, recv, peer):
        return pltpu.make_async_remote_copy(src_ref=src, dst_ref=dst, send_sem=send, recv_sem=recv,
                                            device_id=peer, device_id_type=pl.DeviceIdType.MESH)

    def gather_copy(slot, off, there):
        return remote(kv_s.at[slot, :, own_rows, :], kv_s.at[there, :, own_rows, :],
                      sent_sem.at[0, there], gather_sem.at[there], near(off))

    def cross_copy(slot):
        block = kv_s.at[slot, :, own_rows, :]
        return remote(block, block, sent_sem.at[1, slot], cross_sem.at[slot], sibling)

    def side_copy(slot):
        return remote(part.at[slot, 1 - core], side_in.at[slot], sent_sem.at[1, slot], side_sem.at[slot], sibling)

    def tree_copy(tensor, slot):
        hop = tree.parent(tensor, tree.order[slot])
        return remote(part.at[slot, core, tensor], tree_in.at[tensor, slot],
                      sent_sem.at[2 * tensor, slot], tree_sem.at[tensor, slot], near(hop))

    def concerns(slot, offsets):
        owner = chip_at(tree.order[slot])
        return functools.reduce(jnp.logical_or, [chip_at(o) >= owner for o in offsets])

    def taken(slot, off, there):
        return concerns(slot, [tree.move(off, o) for o in tree.takers(there)])

    def given(tensor, slot, child):
        return concerns(slot, [tree.move(tree.hop_to(slot, child), o) for o in tree.givers(tensor, child)])

    def active(slot):
        return slot_chip(slot) <= mine

    def each_target(slot, act):
        for off, there in tree.targets(slot):
            pl.when(taken(slot, off, there))(functools.partial(act, slot, off, there))

    def arrive(first, last):
        for slot in range(first, last):
            if slot:
                pl.when(concerns(slot, tree.takers(slot)))(
                    gather_copy(slot, tree.source(tree.order[slot]), slot).wait_recv)
            each_target(slot, lambda *which: gather_copy(*which).start())
            pl.when(active(slot))(cross_copy(slot).start)

    xs = sum(o[0] << (2 * i) for i, o in enumerate(tree.order))
    ys = sum(o[1] << (2 * i) for i, o in enumerate(tree.order))

    def slot_chip(slot):
        def field(packed):
            signed = packed - (1 << 32) if packed >= 1 << 31 else packed
            return lax.shift_right_logical(jnp.int32(signed), 2 * slot) & 3
        return chip_at((field(xs), field(ys)))

    def score_step(slot, masked):
        k_blk = kv_s[slot, KEY]
        v_blk = kv_s[slot, VALUE]
        for c, rng in enumerate(chunks):
            s = dot_nn(k_blk, q_t[:, rng])
            if masked:
                key = lax.broadcasted_iota(jnp.int32, s.shape, 0)
                tok = lax.broadcasted_iota(jnp.int32, s.shape, 1) // n_grp + (c * CHUNK // n_grp) + core * c_len
                s = jnp.where(tok >= key, s, NEG_BIG)
            s_buf[slot, :, rng] = s
            m = jnp.max(fold(s), axis=0)
            m_buf[:, rng] = m if masked else jnp.maximum(m_buf[:, rng], m)
            dp_buf[slot, :, rng] = dot_nn(v_blk, do_t[:, rng])

    def value_step(slot):
        v_blk = kv_s[slot, VALUE]
        for rng in chunks:
            w = jnp.exp2(fold(s_buf[slot, :, rng]) * to_log2 - top_buf[:, rng])
            l_buf[:, rng] += jnp.sum(w, axis=0)
            acc_buf[:, rng] += dot_tn(v_blk, w.reshape(width, CHUNK).astype(BF16))

    def top_step(again):
        for rng in chunks:
            top = spread(jnp.max(m_buf[:, rng], axis=0, keepdims=True) * to_log2)
            if again:
                shrink = jnp.exp2(top_buf[:, rng] - top)
                l_buf[:, rng] = l_buf[:, rng] * shrink
                acc_buf[:, rng] = (fold(acc_buf[:, rng]) * shrink).reshape(d_head, CHUNK)
            top_buf[:, rng] = top

    def score_loop(first, last):
        @pl.loop(first, last)
        def _(slot):
            @pl.when(active(slot))
            def _():
                cross_copy(slot).wait_recv()
                score_step(slot, False)

    def value_loop(first, last):
        @pl.loop(first, last)
        def _(slot):
            @pl.when(active(slot))
            def _():
                value_step(slot)
                cross_copy(slot).wait_send()

    loads[0].wait()
    loads[1].wait()
    arrive(0, 1)
    loads[2].wait()
    loads[3].wait()
    with jax.named_scope("first"):
        q_t[...] = q_s[...].astype(F32).T.astype(BF16)
        do_t[...] = do_s[...].astype(F32).T.astype(BF16)
        l_buf[...] = jnp.zeros(l_buf.shape, F32)
        acc_buf[...] = jnp.zeros(acc_buf.shape, F32)
        cross_copy(0).wait_recv()
        score_step(0, True)

    n_next = len(tree.hops) + 1
    with jax.named_scope("arrive_next"):
        arrive(1, n_next)
    with jax.named_scope("score_next"):
        score_loop(1, n_next)
    with jax.named_scope("arrive_near"):
        arrive(n_next, n_near)
    with jax.named_scope("score_near"):
        score_loop(n_next, n_near)
    with jax.named_scope("value_near"):
        top_step(False)
        value_loop(0, n_near)
    with jax.named_scope("arrive_far"):
        arrive(n_near, n_slot)
    with jax.named_scope("score_far"):
        score_loop(n_near, n_slot)
    with jax.named_scope("value_far"):
        top_step(True)
        value_loop(n_near, n_slot)

    with jax.named_scope("out"):
        for rng in chunks:
            l = spread(jnp.sum(l_buf[:, rng], axis=0, keepdims=True))
            out = (fold(acc_buf[:, rng]) / l).reshape(d_head, CHUNK).astype(BF16).astype(F32)
            o_out[rng, :] = out.T.astype(BF16)
            top_buf[:, rng] = top_buf[:, rng] + jnp.log2(l)
            d_buf[:, rng] = spread(jnp.sum(do_t[:, rng].astype(F32) * out, axis=0, keepdims=True))
        acc_buf[...] = jnp.zeros(acc_buf.shape, F32)
        for slot in range(n_near):
            each_target(slot, lambda *which: gather_copy(*which).wait_send())

    def grad_step(slot):
        dv = jnp.zeros((width, d_head), F32)
        dk = jnp.zeros((width, d_head), F32)
        for rng in chunks:
            p = jnp.exp2(fold(s_buf[slot, :, rng]) * to_log2 - top_buf[:, rng])
            ds = p * (fold(dp_buf[slot, :, rng]) - d_buf[:, rng])
            ds = ds.reshape(width, CHUNK).astype(BF16)
            ds_buf[slot, :, rng] = ds
            dv = dv + dot_nn(p.reshape(width, CHUNK).astype(BF16), do_s[rng, :])
            dk = dk + dot_nn(ds, q_s[rng, :])
        for h in range(2):
            part[slot, h, KEY] = dk[h * c_len:(h + 1) * c_len, :]
            part[slot, h, VALUE] = dv[h * c_len:(h + 1) * c_len, :]

    def zero_step(slot):
        part[slot] = jnp.zeros(part.shape[1:], F32)

    def merge(slot):
        @pl.when(active(slot))
        def _():
            side_copy(slot).wait_recv()
            part[slot, core] = part[slot, core] + side_in[slot]

        for tensor in (KEY, VALUE):
            for child in tree.children(tensor, tree.order[slot]):
                @pl.when(given(tensor, slot, child))
                def _():
                    tree_copy(tensor, child).wait_recv()
                    part[slot, core, tensor] = part[slot, core, tensor] + tree_in[tensor, child]
            if slot:
                pl.when(concerns(slot, tree.givers(tensor, slot)))(tree_copy(tensor, slot).start)
        if slot == 0:
            dk_out[...] = (part[0, core, KEY] * scale).astype(BF16)
            dv_out[...] = part[0, core, VALUE].astype(BF16)

    def sums_sent(first, last):
        for slot in range(first, last):
            for tensor in (KEY, VALUE):
                pl.when(concerns(slot, tree.givers(tensor, slot)))(tree_copy(tensor, slot).wait_send)

    def query_step(slot):
        k_blk = kv_s[slot, KEY]
        for rng in chunks:
            acc_buf[:, rng] += dot_tn(k_blk, ds_buf[slot, :, rng])

    def query_loop(first, last):
        if first < last:
            with jax.named_scope(f"query#n={last - first}"):
                @pl.loop(first, last)
                def _(slot):
                    pl.when(active(slot))(lambda: query_step(slot))

    left = n_slot
    before = {}
    for slot in reversed(range(n_slot)):
        taken = min(QUERIES.get(slot, 0), left)
        before[slot] = (left - taken, left)
        left -= taken

    def merge_after_queries(slot):
        query_loop(*before[slot])
        with jax.named_scope(f"merge#s={slot}"):
            merge(slot)

    @pl.loop(0, n_slot)
    def _(step):
        slot = n_slot - 1 - step

        @pl.when(active(slot))
        def _():
            with jax.named_scope("grad"):
                grad_step(slot)
            side_copy(slot).start()

        pl.when(jnp.logical_not(active(slot)))(lambda: zero_step(slot))
        for s in range(LAG, n_slot):
            pl.when(slot == s - LAG)(functools.partial(merge_after_queries, s))

    for s in reversed(range(1, LAG)):
        merge_after_queries(s)
    query_loop(0, left)
    with jax.named_scope("query_out"):
        for rng in chunks:
            dq_out[rng, :] = (acc_buf[:, rng] * scale).T.astype(BF16)
    with jax.named_scope("drain"):
        sums_sent(len(tree.hops) + 1, n_slot)

        @pl.loop(0, n_slot)
        def _(slot):
            pl.when(active(slot))(lambda: side_copy(slot).wait_send())

    with jax.named_scope("merge#s=0"):
        merge(0)
    sums_sent(1, len(tree.hops) + 1)


def store_kernel(*refs):
    *pairs, sem = refs
    half = len(pairs) // 2
    copies = [pltpu.make_async_copy(src, dst, sem.at[i]) for i, (src, dst) in enumerate(zip(pairs[:half], pairs[half:]))]
    for copy in copies:
        copy.start()
    for copy in copies:
        copy.wait()


def solution(mesh):
    part_spec = P("dp", "ctx")
    n_dev = mesh.shape["ctx"]
    tree = Tree(math.isqrt(n_dev // 2))

    def local_step(queries, keys, values, grad_out):
        n_batch, c_len, n_q, d_head = queries.shape
        n_kv = keys.shape[2]
        n_grp = n_q // n_kv
        rows = c_len * n_q
        width = 2 * c_len
        n_slot = n_dev // 2
        scale = d_head ** -0.5
        any_spec = pl.BlockSpec(memory_space=pl.ANY)
        dma_sem = pltpu.SemaphoreType.DMA
        shapes = [(rows, d_head)] * 2 + [(c_len, d_head)] * 2
        results = pl.pallas_call(
            functools.partial(attn_kernel, tree, n_grp, scale),
            out_shape=[pltpu.VMEM(shape, BF16) for shape in shapes],
            in_specs=[any_spec] * 4,
            out_specs=[pl.BlockSpec(memory_space=pltpu.VMEM)] * 4,
            scratch_shapes=[
                pltpu.VMEM((rows, d_head), BF16),
                pltpu.VMEM((rows, d_head), BF16),
                pltpu.VMEM((n_slot, 2, width, d_head), BF16),
                pltpu.VMEM((d_head, rows), BF16),
                pltpu.VMEM((d_head, rows), BF16),
                pltpu.VMEM((n_slot, width, rows), F32),
                pltpu.VMEM((n_slot, width, rows), F32),
                pltpu.VMEM((n_slot, width, rows), BF16),
                pltpu.VMEM((SUBLANES, rows), F32),
                pltpu.VMEM((SUBLANES, rows), F32),
                pltpu.VMEM((SUBLANES, rows), F32),
                pltpu.VMEM((d_head, rows), F32),
                pltpu.VMEM((SUBLANES, rows), F32),
                pltpu.VMEM((n_slot, 2, 2, c_len, d_head), F32),
                pltpu.VMEM((n_slot, 2, c_len, d_head), F32),
                pltpu.VMEM((2, n_slot, c_len, d_head), F32),
                dma_sem((4,)),
                dma_sem((n_slot,)),
                dma_sem((n_slot,)),
                dma_sem((n_slot,)),
                dma_sem((2, n_slot)),
                dma_sem((3, n_slot)),
            ],
            compiler_params=pltpu.CompilerParams(
                vmem_limit_bytes=60 * 1024 * 1024, collective_id=0, has_side_effects=True),
            name="attn",
        )(queries.reshape(rows, d_head), grad_out.reshape(rows, d_head),
          keys.reshape(c_len, d_head), values.reshape(c_len, d_head))
        out, dq, dk, dv = pl.pallas_call(
            store_kernel,
            out_shape=[jax.ShapeDtypeStruct(shape, BF16) for shape in shapes],
            in_specs=[pl.BlockSpec(memory_space=pltpu.VMEM)] * 4,
            out_specs=[any_spec] * 4,
            scratch_shapes=[dma_sem((4,))],
            compiler_params=pltpu.CompilerParams(vmem_limit_bytes=2 * 1024 * 1024),
            name="store",
        )(*results)
        q_shape = (n_batch, c_len, n_q, d_head)
        kv_shape = (n_batch, c_len, n_kv, d_head)
        return out.reshape(q_shape), dq.reshape(q_shape), dk.reshape(kv_shape), dv.reshape(kv_shape)

    return jax.shard_map(local_step, mesh=mesh, in_specs=(part_spec,) * 4, out_specs=(part_spec,) * 4, check_vma=False)
```

```python
import functools
import math

import jax
import jax.numpy as jnp
from jax import lax
from jax.experimental import pallas as pl
from jax.experimental.pallas import tpu as pltpu
from jax.sharding import PartitionSpec as P

NEG_BIG = -1e30
CHUNK = 256
SUBLANES = 8
KEY, VALUE = 0, 1
F32 = jnp.float32
BF16 = jnp.bfloat16
GRAD, SUM, QUERY = 0, 1, 2
PLAN = (
    (GRAD, 15), (GRAD, 11), (GRAD, 7), (GRAD, 12), (SUM, 15), (SUM, 11), (GRAD, 13), (GRAD, 10), (SUM, 12),
    (GRAD, 9), (SUM, 13), (QUERY, 2), (SUM, 10), (GRAD, 3), (SUM, 7), (SUM, 9), (GRAD, 14), (GRAD, 1), (GRAD, 8),
    (SUM, 14), (SUM, 1), (QUERY, 2), (GRAD, 5), (GRAD, 2), (SUM, 8), (GRAD, 0), (SUM, 5), (GRAD, 6), (GRAD, 4),
    (QUERY, 2), (SUM, 6), (QUERY, 2), (QUERY, 2), (SUM, 2), (SUM, 4), (QUERY, 2), (QUERY, 2), (QUERY, 2), (SUM, 3),
)
PARENTS = (
    (None, (0, 1), (0, 3), (1, 0), (3, 0), (1, 1), (0, 3), (0, 1), (3, 0), (0, 3), (1, 0), (0, 1), (1, 0), (3, 0), (3, 3), (1, 1)),
    (None, (0, 1), (0, 3), (1, 0), (3, 0), (1, 1), (1, 3), (0, 1), (3, 0), (0, 3), (3, 0), (0, 3), (1, 0), (1, 0), (3, 3), (3, 3)),
)


def dot_tn(a, b):
    return lax.dot_general(a, b, (((0,), (0,)), ((), ())), preferred_element_type=F32)


def dot_nn(a, b):
    return jnp.dot(a, b, preferred_element_type=F32)


def fold(x):
    return x.reshape(x.shape[0] // SUBLANES, SUBLANES, x.shape[1])


def spread(x):
    return jnp.broadcast_to(x, (SUBLANES, x.shape[1]))


class Tree:
    def __init__(self, side):
        self.side = side
        offsets = [(dx, dy) for dx in range(side) for dy in range(side)]
        mid = side // 2

        def group(o):
            if mid in o:
                return 3 if 0 in o else 5 if o == (mid, mid) else 4
            return 0 if o == (0, 0) else 1 if 0 in o else 2

        self.order = sorted(offsets, key=lambda o: (group(o), o))
        kinds = [group(o) for o in self.order]
        self.bounds = [kinds.index(k) for k in range(5)] + [len(kinds)]
        self.n_near = self.bounds[3]
        self.slot = {o: i for i, o in enumerate(self.order)}

    def parent(self, tensor, off):
        return PARENTS[tensor][self.slot[off]]

    def children(self, tensor, off):
        return [there for there in range(1, len(self.order)) if off == tuple(
            (o - p) % self.side for o, p in zip(self.order[there], self.parent(tensor, self.order[there])))]

    def source(self, off):
        side = self.side
        mid, one, far = side // 2, 1, side - 1
        if mid not in off:
            return off
        if off == (mid, mid):
            return (one, one)
        if off[0] == mid:
            return (one if off[1] == 0 else far, 0)
        return (0, one if off[0] == 0 else far)

    def targets(self, slot):
        found = []
        for there in range(1, len(self.order)):
            src = self.source(self.order[there])
            if tuple((o - e) % self.side for o, e in zip(self.order[there], src)) == self.order[slot]:
                found.append((tuple((-e) % self.side for e in src), there))
        return found


    def takers(self, slot):
        found = [(0, 0)]
        for off, there in self.targets(slot):
            found += [self.move(off, o) for o in self.takers(there)]
        return found

    def givers(self, tensor, slot):
        found = [(0, 0)]
        for child in self.children(tensor, self.order[slot]):
            hop = self.hop_to(slot, child)
            found += [self.move(hop, o) for o in self.givers(tensor, child)]
        return found

    def move(self, a, b):
        return tuple((i + j) % self.side for i, j in zip(a, b))

    def hop_to(self, slot, child):
        return tuple((i - j) % self.side for i, j in zip(self.order[slot], self.order[child]))


def attn_kernel(tree, n_grp, scale, q_hbm, do_hbm, k_hbm, v_hbm, o_out, dq_out, dk_out, dv_out,
                q_s, do_s, kv_s, q_t, do_t, s_buf, dp_buf, ds_buf, p_buf, m_buf, top_buf, l_buf, acc_buf, d_buf,
                part, side_in, tree_in, local_sem, gather_sem, cross_sem, side_sem, tree_sem, sent_sem):
    rows, d_head = q_s.shape
    c_len = k_hbm.shape[0]
    width = 2 * c_len
    side = tree.side
    n_slot = side * side
    n_near = tree.n_near
    dev = lax.axis_index("ctx")
    core = lax.rem(dev, 2)
    mine = dev // 2
    at_x = lax.rem(mine, side)
    at_y = mine // side
    sibling = {"ctx": mine * 2 + 1 - core}
    chunks = [pl.ds(i * CHUNK, CHUNK) for i in range(rows // CHUNK)]
    to_log2 = scale * math.log2(math.e)
    own_rows = pl.ds(pl.multiple_of(core * c_len, c_len), c_len)

    def chip_at(off):
        return lax.rem(at_y + off[1], side) * side + lax.rem(at_x + off[0], side)

    def near(off):
        return {"ctx": chip_at(off) * 2 + core}

    loads = [
        pltpu.make_async_copy(k_hbm, kv_s.at[0, KEY, own_rows, :], local_sem.at[0]),
        pltpu.make_async_copy(v_hbm, kv_s.at[0, VALUE, own_rows, :], local_sem.at[1]),
        pltpu.make_async_copy(q_hbm, q_s, local_sem.at[2]),
        pltpu.make_async_copy(do_hbm, do_s, local_sem.at[3]),
    ]
    for copy in loads:
        copy.start()

    with jax.named_scope("barrier"):
        barrier = pltpu.get_barrier_semaphore()
        peers = [near(off) for off in tree.order[1:n_near]] + [sibling]
        for peer in peers:
            pl.semaphore_signal(barrier, inc=1, device_id=peer, device_id_type=pl.DeviceIdType.MESH)
        pl.semaphore_wait(barrier, len(peers))

    def remote(src, dst, send, recv, peer):
        return pltpu.make_async_remote_copy(src_ref=src, dst_ref=dst, send_sem=send, recv_sem=recv,
                                            device_id=peer, device_id_type=pl.DeviceIdType.MESH)

    def gather_copy(slot, off, there):
        return remote(kv_s.at[slot, :, own_rows, :], kv_s.at[there, :, own_rows, :],
                      sent_sem.at[0, there], gather_sem.at[there], near(off))

    def cross_copy(slot):
        block = kv_s.at[slot, :, own_rows, :]
        return remote(block, block, sent_sem.at[1, slot], cross_sem.at[slot], sibling)

    def side_copy(slot):
        return remote(part.at[slot, 1 - core], side_in.at[slot], sent_sem.at[1, slot], side_sem.at[slot], sibling)

    def tree_copy(tensor, slot):
        hop = tree.parent(tensor, tree.order[slot])
        return remote(part.at[slot, core, tensor], tree_in.at[tensor, slot],
                      sent_sem.at[2 * tensor, slot], tree_sem.at[tensor, slot], near(hop))

    def concerns(slot, offsets):
        owner = chip_at(tree.order[slot])
        return functools.reduce(jnp.logical_or, [chip_at(o) >= owner for o in offsets])

    def taken(slot, off, there):
        return concerns(slot, [tree.move(off, o) for o in tree.takers(there)])

    def given(tensor, slot, child):
        return concerns(slot, [tree.move(tree.hop_to(slot, child), o) for o in tree.givers(tensor, child)])

    def active(slot):
        owner = chip_at(tree.order[slot]) if isinstance(slot, int) else slot_chip(slot)
        return owner <= mine

    def each_target(slot, act):
        for off, there in tree.targets(slot):
            pl.when(taken(slot, off, there))(functools.partial(act, slot, off, there))

    def arrive(first, last):
        for slot in range(first, last):
            if slot:
                pl.when(concerns(slot, tree.takers(slot)))(
                    gather_copy(slot, tree.source(tree.order[slot]), slot).wait_recv)
            each_target(slot, lambda *which: gather_copy(*which).start())
            pl.when(active(slot))(cross_copy(slot).start)

    xs = sum(o[0] << (2 * i) for i, o in enumerate(tree.order))
    ys = sum(o[1] << (2 * i) for i, o in enumerate(tree.order))

    def slot_chip(slot):
        def field(packed):
            signed = packed - (1 << 32) if packed >= 1 << 31 else packed
            return lax.shift_right_logical(jnp.int32(signed), 2 * slot) & 3
        return chip_at((field(xs), field(ys)))

    def score_step(slots, masked):
        for c, rng in enumerate(chunks):
            m = None if masked else m_buf[:, rng]
            for slot in slots:
                s = dot_nn(kv_s[slot, KEY], q_t[:, rng])
                if masked:
                    key = lax.broadcasted_iota(jnp.int32, s.shape, 0)
                    tok = lax.broadcasted_iota(jnp.int32, s.shape, 1) // n_grp + (c * CHUNK // n_grp) + core * c_len
                    s = jnp.where(tok >= key, s, NEG_BIG)
                s_buf[slot, :, rng] = s
                top = jnp.max(fold(s), axis=0)
                m = top if m is None else jnp.maximum(m, top)
                dp_buf[slot, :, rng] = dot_nn(kv_s[slot, VALUE], do_t[:, rng])
            m_buf[:, rng] = m

    def value_step(slots):
        for rng in chunks:
            l = l_buf[:, rng]
            acc = acc_buf[:, rng]
            for slot in slots:
                w = jnp.exp2(fold(s_buf[slot, :, rng]) * to_log2 - top_buf[:, rng])
                l = l + jnp.sum(w, axis=0)
                acc = acc + dot_tn(kv_s[slot, VALUE], w.reshape(width, CHUNK).astype(BF16))
            l_buf[:, rng] = l
            acc_buf[:, rng] = acc

    def top_step(again):
        for rng in chunks:
            top = spread(jnp.max(m_buf[:, rng], axis=0, keepdims=True) * to_log2)
            if again:
                shrink = jnp.exp2(top_buf[:, rng] - top)
                l_buf[:, rng] = l_buf[:, rng] * shrink
                acc_buf[:, rng] = (fold(acc_buf[:, rng]) * shrink).reshape(d_head, CHUNK)
            top_buf[:, rng] = top

    def pair_loop(first, last, body):
        @pl.loop(0, (last - first) // 2)
        def _(i):
            a, b = first + 2 * i, first + 2 * i + 1
            both = jnp.logical_and(active(a), active(b))
            pl.when(both)(lambda: body([a, b]))
            for slot in (a, b):
                pl.when(jnp.logical_and(active(slot), jnp.logical_not(both)))(functools.partial(body, [slot]))

        if (last - first) % 2:
            pl.when(active(last - 1))(lambda: body([last - 1]))

    def score_body(slots):
        for slot in slots:
            cross_copy(slot).wait_recv()
        score_step(slots, False)

    def value_body(slots):
        value_step(slots)
        for slot in slots:
            cross_copy(slot).wait_send()

    def score_loop(first, last):
        pair_loop(first, last, score_body)

    def value_loop(first, last):
        pair_loop(first, last, value_body)

    loads[0].wait()
    loads[1].wait()
    arrive(0, 1)
    loads[2].wait()
    loads[3].wait()
    with jax.named_scope("first"):
        q_t[...] = q_s[...].astype(F32).T.astype(BF16)
        do_t[...] = do_s[...].astype(F32).T.astype(BF16)
        l_buf[...] = jnp.zeros(l_buf.shape, F32)
        acc_buf[...] = jnp.zeros(acc_buf.shape, F32)
        cross_copy(0).wait_recv()
        score_step([0], True)

    n_next = tree.bounds[2]
    for first, last in ((1, n_next), (n_next, n_near)):
        with jax.named_scope(f"arrive#s={first}"):
            arrive(first, last)
        with jax.named_scope(f"score#s={first}"):
            score_loop(first, last)
    with jax.named_scope("value_near"):
        top_step(False)
        value_loop(0, n_near)
    with jax.named_scope("arrive_far"):
        arrive(n_near, n_slot)
    with jax.named_scope("score_far"):
        score_loop(n_near, n_slot)
    with jax.named_scope("value_far"):
        top_step(True)
        value_loop(n_near, n_slot)

    with jax.named_scope("out"):
        for rng in chunks:
            l = spread(jnp.sum(l_buf[:, rng], axis=0, keepdims=True))
            out = (fold(acc_buf[:, rng]) / l).reshape(d_head, CHUNK).astype(BF16).astype(F32)
            o_out[rng, :] = out.T.astype(BF16)
            top_buf[:, rng] = top_buf[:, rng] + jnp.log2(l)
            d_buf[:, rng] = spread(jnp.sum(do_t[:, rng].astype(F32) * out, axis=0, keepdims=True))
        acc_buf[...] = jnp.zeros(acc_buf.shape, F32)
        for slot in range(n_near):
            each_target(slot, lambda *which: gather_copy(*which).wait_send())

    def grad_step(slot):
        for rng in chunks:
            p = jnp.exp2(fold(s_buf[slot, :, rng]) * to_log2 - top_buf[:, rng])
            ds = p * (fold(dp_buf[slot, :, rng]) - d_buf[:, rng])
            p_buf[:, rng] = p.reshape(width, CHUNK).astype(BF16)
            ds_buf[slot, :, rng] = ds.reshape(width, CHUNK).astype(BF16)
        for h in range(2):
            keys = pl.ds(h * c_len, c_len)
            part[slot, h, KEY] = dot_nn(ds_buf[slot, keys, :], q_s[...])
            part[slot, h, VALUE] = dot_nn(p_buf[keys, :], do_s[...])

    def zero_step(slot):
        part[slot] = jnp.zeros(part.shape[1:], F32)

    def merge(slot):
        @pl.when(active(slot))
        def _():
            side_copy(slot).wait_recv()
            part[slot, core] = part[slot, core] + side_in[slot]

        for tensor in (KEY, VALUE):
            for child in tree.children(tensor, tree.order[slot]):
                @pl.when(given(tensor, slot, child))
                def _():
                    tree_copy(tensor, child).wait_recv()
                    part[slot, core, tensor] = part[slot, core, tensor] + tree_in[tensor, child]
            if slot:
                pl.when(concerns(slot, tree.givers(tensor, slot)))(tree_copy(tensor, slot).start)
        if slot == 0:
            dk_out[...] = (part[0, core, KEY] * scale).astype(BF16)
            dv_out[...] = part[0, core, VALUE].astype(BF16)

    def sums_sent(slots):
        for slot in slots:
            for tensor in (KEY, VALUE):
                pl.when(concerns(slot, tree.givers(tensor, slot)))(tree_copy(tensor, slot).wait_send)

    def query_step(slots):
        for rng in chunks:
            acc = acc_buf[:, rng]
            for slot in slots:
                acc = acc + dot_tn(kv_s[slot, KEY], ds_buf[slot, :, rng])
            acc_buf[:, rng] = acc

    def queries(slots):
        for a, b in zip(slots[::2], slots[1::2]):
            both = jnp.logical_and(active(a), active(b))
            pl.when(both)(functools.partial(query_step, [a, b]))
            for slot in (a, b):
                pl.when(jnp.logical_and(active(slot), jnp.logical_not(both)))(functools.partial(query_step, [slot]))
        if len(slots) % 2:
            pl.when(active(slots[-1]))(functools.partial(query_step, [slots[-1]]))

    order = [which for what, which in PLAN if what == GRAD]
    sums = [which for what, which in PLAN if what == SUM]
    asked = 0
    for what, which in PLAN:
        if what == GRAD:
            with jax.named_scope(f"grad#s={which}"):
                pl.when(active(which))(functools.partial(grad_step, which))
                pl.when(jnp.logical_not(active(which)))(functools.partial(zero_step, which))
            pl.when(active(which))(side_copy(which).start)
        elif what == SUM:
            with jax.named_scope(f"merge#s={which}"):
                merge(which)
        else:
            with jax.named_scope(f"query#n={which}"):
                queries(order[asked:asked + which])
            asked += which

    with jax.named_scope("query"):
        queries(order[asked:])
        for rng in chunks:
            dq_out[rng, :] = (acc_buf[:, rng] * scale).T.astype(BF16)
    with jax.named_scope("drain"):
        sums_sent(sums[:-4])

        @pl.loop(0, n_slot)
        def _(slot):
            pl.when(active(slot))(lambda: side_copy(slot).wait_send())

    with jax.named_scope("merge#s=0"):
        merge(0)
    sums_sent(sums[-4:])


def store_kernel(*refs):
    *pairs, sem = refs
    half = len(pairs) // 2
    copies = [pltpu.make_async_copy(src, dst, sem.at[i]) for i, (src, dst) in enumerate(zip(pairs[:half], pairs[half:]))]
    for copy in copies:
        copy.start()
    for copy in copies:
        copy.wait()


def solution(mesh):
    part_spec = P("dp", "ctx")
    n_dev = mesh.shape["ctx"]
    tree = Tree(math.isqrt(n_dev // 2))

    def local_step(queries, keys, values, grad_out):
        n_batch, c_len, n_q, d_head = queries.shape
        n_kv = keys.shape[2]
        n_grp = n_q // n_kv
        rows = c_len * n_q
        width = 2 * c_len
        n_slot = n_dev // 2
        scale = d_head ** -0.5
        any_spec = pl.BlockSpec(memory_space=pl.ANY)
        dma_sem = pltpu.SemaphoreType.DMA
        shapes = [(rows, d_head)] * 2 + [(c_len, d_head)] * 2
        results = pl.pallas_call(
            functools.partial(attn_kernel, tree, n_grp, scale),
            out_shape=[pltpu.VMEM(shape, BF16) for shape in shapes],
            in_specs=[any_spec] * 4,
            out_specs=[pl.BlockSpec(memory_space=pltpu.VMEM)] * 4,
            scratch_shapes=[
                pltpu.VMEM((rows, d_head), BF16),
                pltpu.VMEM((rows, d_head), BF16),
                pltpu.VMEM((n_slot, 2, width, d_head), BF16),
                pltpu.VMEM((d_head, rows), BF16),
                pltpu.VMEM((d_head, rows), BF16),
                pltpu.VMEM((n_slot, width, rows), F32),
                pltpu.VMEM((n_slot, width, rows), F32),
                pltpu.VMEM((n_slot, width, rows), BF16),
                pltpu.VMEM((width, rows), BF16),
                pltpu.VMEM((SUBLANES, rows), F32),
                pltpu.VMEM((SUBLANES, rows), F32),
                pltpu.VMEM((SUBLANES, rows), F32),
                pltpu.VMEM((d_head, rows), F32),
                pltpu.VMEM((SUBLANES, rows), F32),
                pltpu.VMEM((n_slot, 2, 2, c_len, d_head), F32),
                pltpu.VMEM((n_slot, 2, c_len, d_head), F32),
                pltpu.VMEM((2, n_slot, c_len, d_head), F32),
                dma_sem((4,)),
                dma_sem((n_slot,)),
                dma_sem((n_slot,)),
                dma_sem((n_slot,)),
                dma_sem((2, n_slot)),
                dma_sem((3, n_slot)),
            ],
            compiler_params=pltpu.CompilerParams(
                vmem_limit_bytes=60 * 1024 * 1024, collective_id=0, has_side_effects=True),
            name="attn",
        )(queries.reshape(rows, d_head), grad_out.reshape(rows, d_head),
          keys.reshape(c_len, d_head), values.reshape(c_len, d_head))
        out, dq, dk, dv = pl.pallas_call(
            store_kernel,
            out_shape=[jax.ShapeDtypeStruct(shape, BF16) for shape in shapes],
            in_specs=[pl.BlockSpec(memory_space=pltpu.VMEM)] * 4,
            out_specs=[any_spec] * 4,
            scratch_shapes=[dma_sem((4,))],
            compiler_params=pltpu.CompilerParams(vmem_limit_bytes=2 * 1024 * 1024),
            name="store",
        )(*results)
        q_shape = (n_batch, c_len, n_q, d_head)
        kv_shape = (n_batch, c_len, n_kv, d_head)
        return out.reshape(q_shape), dq.reshape(q_shape), dk.reshape(kv_shape), dv.reshape(kv_shape)

    return jax.shard_map(local_step, mesh=mesh, in_specs=(part_spec,) * 4, out_specs=(part_spec,) * 4, check_vma=False)
```

```python
import functools
import math

import jax
import jax.numpy as jnp
from jax import lax
from jax.experimental import pallas as pl
from jax.experimental.pallas import tpu as pltpu
from jax.sharding import PartitionSpec as P

NEG_BIG = -1e30
CHUNK = 256
SUBLANES = 8
KEY, VALUE = 0, 1
F32 = jnp.float32
BF16 = jnp.bfloat16
GRAD, SUM, QUERY = 0, 1, 2
PLAN = (
    (GRAD, 15), (GRAD, 11), (GRAD, 12), (SUM, 15), (GRAD, 13), (SUM, 11), (GRAD, 7), (SUM, 12), (GRAD, 14),
    (SUM, 13), (GRAD, 9), (GRAD, 1), (SUM, 7), (SUM, 14), (GRAD, 10), (SUM, 9), (QUERY, 2), (SUM, 1), (QUERY, 2),
    (QUERY, 2), (QUERY, 2), (SUM, 10), (GRAD, 5), (GRAD, 4), (GRAD, 8), (GRAD, 6), (QUERY, 2), (SUM, 5), (SUM, 8),
    (QUERY, 2), (GRAD, 3), (SUM, 6), (GRAD, 2), (QUERY, 2), (GRAD, 0), (SUM, 2), (SUM, 4), (QUERY, 2), (SUM, 3),
)
PARENTS = (
    (None, (0, 1), (0, 3), (1, 0), (3, 0), (1, 1), (0, 3), (0, 1), (3, 0), (0, 3), (1, 0), (0, 1), (1, 0), (3, 0), (3, 3), (1, 1)),
    (None, (0, 1), (0, 3), (1, 0), (3, 0), (1, 1), (1, 3), (0, 1), (3, 0), (0, 3), (3, 0), (0, 3), (1, 0), (1, 0), (3, 3), (3, 3)),
)


def dot_tn(a, b):
    return lax.dot_general(a, b, (((0,), (0,)), ((), ())), preferred_element_type=F32)


def dot_nn(a, b):
    return jnp.dot(a, b, preferred_element_type=F32)


def fold(x):
    return x.reshape(x.shape[0] // SUBLANES, SUBLANES, x.shape[1])


def spread(x):
    return jnp.broadcast_to(x, (SUBLANES, x.shape[1]))


class Tree:
    def __init__(self, side):
        self.side = side
        offsets = [(dx, dy) for dx in range(side) for dy in range(side)]
        mid = side // 2

        def group(o):
            if mid in o:
                return 3 if 0 in o else 5 if o == (mid, mid) else 4
            return 0 if o == (0, 0) else 1 if 0 in o else 2

        self.order = sorted(offsets, key=lambda o: (group(o), o))
        kinds = [group(o) for o in self.order]
        self.bounds = [kinds.index(k) for k in range(5)] + [len(kinds)]
        self.n_near = self.bounds[3]
        self.slot = {o: i for i, o in enumerate(self.order)}

    def parent(self, tensor, off):
        return PARENTS[tensor][self.slot[off]]

    def children(self, tensor, off):
        return [there for there in range(1, len(self.order)) if off == tuple(
            (o - p) % self.side for o, p in zip(self.order[there], self.parent(tensor, self.order[there])))]

    def source(self, off):
        side = self.side
        mid, one, far = side // 2, 1, side - 1
        if mid not in off:
            return off
        if off == (mid, mid):
            return (one, one)
        if off[0] == mid:
            return (one if off[1] == 0 else far, 0)
        return (0, one if off[0] == 0 else far)

    def targets(self, slot):
        found = []
        for there in range(1, len(self.order)):
            src = self.source(self.order[there])
            if tuple((o - e) % self.side for o, e in zip(self.order[there], src)) == self.order[slot]:
                found.append((tuple((-e) % self.side for e in src), there))
        return found


    def takers(self, slot):
        found = [(0, 0)]
        for off, there in self.targets(slot):
            found += [self.move(off, o) for o in self.takers(there)]
        return found

    def givers(self, tensor, slot):
        found = [(0, 0)]
        for child in self.children(tensor, self.order[slot]):
            hop = self.hop_to(slot, child)
            found += [self.move(hop, o) for o in self.givers(tensor, child)]
        return found

    def move(self, a, b):
        return tuple((i + j) % self.side for i, j in zip(a, b))

    def hop_to(self, slot, child):
        return tuple((i - j) % self.side for i, j in zip(self.order[slot], self.order[child]))


def attn_kernel(tree, n_grp, scale, q_hbm, do_hbm, k_hbm, v_hbm, o_out, dq_out, dk_out, dv_out,
                q_s, do_s, kv_s, q_t, do_t, s_buf, dp_buf, ds_buf, p_buf, m_buf, top_buf, l_buf, acc_buf, d_buf,
                part, side_in, tree_in, local_sem, gather_sem, cross_sem, side_sem, tree_sem, sent_sem):
    rows, d_head = q_s.shape
    c_len = k_hbm.shape[0]
    width = 2 * c_len
    side = tree.side
    n_slot = side * side
    n_near = tree.n_near
    dev = lax.axis_index("ctx")
    core = lax.rem(dev, 2)
    mine = dev // 2
    at_x = lax.rem(mine, side)
    at_y = mine // side
    sibling = {"ctx": mine * 2 + 1 - core}
    chunks = [pl.ds(i * CHUNK, CHUNK) for i in range(rows // CHUNK)]
    to_log2 = scale * math.log2(math.e)
    own_rows = pl.ds(pl.multiple_of(core * c_len, c_len), c_len)

    def chip_at(off):
        return lax.rem(at_y + off[1], side) * side + lax.rem(at_x + off[0], side)

    def near(off):
        return {"ctx": chip_at(off) * 2 + core}

    loads = [
        pltpu.make_async_copy(k_hbm, kv_s.at[0, KEY, own_rows, :], local_sem.at[0]),
        pltpu.make_async_copy(v_hbm, kv_s.at[0, VALUE, own_rows, :], local_sem.at[1]),
        pltpu.make_async_copy(q_hbm, q_s, local_sem.at[2]),
        pltpu.make_async_copy(do_hbm, do_s, local_sem.at[3]),
    ]
    for copy in loads:
        copy.start()

    with jax.named_scope("barrier"):
        barrier = pltpu.get_barrier_semaphore()
        peers = [near(off) for off in tree.order[1:n_near]] + [sibling]
        for peer in peers:
            pl.semaphore_signal(barrier, inc=1, device_id=peer, device_id_type=pl.DeviceIdType.MESH)
        pl.semaphore_wait(barrier, len(peers))

    def remote(src, dst, send, recv, peer):
        return pltpu.make_async_remote_copy(src_ref=src, dst_ref=dst, send_sem=send, recv_sem=recv,
                                            device_id=peer, device_id_type=pl.DeviceIdType.MESH)

    def gather_copy(slot, off, there):
        return remote(kv_s.at[slot, :, own_rows, :], kv_s.at[there, :, own_rows, :],
                      sent_sem.at[0, there], gather_sem.at[there], near(off))

    def cross_copy(slot):
        block = kv_s.at[slot, :, own_rows, :]
        return remote(block, block, sent_sem.at[1, slot], cross_sem.at[slot], sibling)

    def side_copy(slot):
        return remote(part.at[slot, 1 - core], side_in.at[slot], sent_sem.at[1, slot], side_sem.at[slot], sibling)

    def tree_copy(tensor, slot):
        hop = tree.parent(tensor, tree.order[slot])
        return remote(part.at[slot, core, tensor], tree_in.at[tensor, slot],
                      (gather_sem, cross_sem)[tensor].at[slot], tree_sem.at[tensor, slot], near(hop))

    def concerns(slot, offsets):
        owner = chip_at(tree.order[slot])
        return functools.reduce(jnp.logical_or, [chip_at(o) >= owner for o in offsets])

    def taken(slot, off, there):
        return concerns(slot, [tree.move(off, o) for o in tree.takers(there)])

    def given(tensor, slot, child):
        return concerns(slot, [tree.move(tree.hop_to(slot, child), o) for o in tree.givers(tensor, child)])

    def active(slot):
        owner = chip_at(tree.order[slot]) if isinstance(slot, int) else slot_chip(slot)
        return owner <= mine

    def each_target(slot, act):
        for off, there in tree.targets(slot):
            pl.when(taken(slot, off, there))(functools.partial(act, slot, off, there))

    def arrive(first, last):
        for slot in range(first, last):
            if slot:
                pl.when(concerns(slot, tree.takers(slot)))(
                    gather_copy(slot, tree.source(tree.order[slot]), slot).wait_recv)
            each_target(slot, lambda *which: gather_copy(*which).start())
            pl.when(active(slot))(cross_copy(slot).start)

    xs = sum(o[0] << (2 * i) for i, o in enumerate(tree.order))
    ys = sum(o[1] << (2 * i) for i, o in enumerate(tree.order))

    def slot_chip(slot):
        def field(packed):
            signed = packed - (1 << 32) if packed >= 1 << 31 else packed
            return lax.shift_right_logical(jnp.int32(signed), 2 * slot) & 3
        return chip_at((field(xs), field(ys)))

    def score_step(slots, masked, with_dp):
        for c, rng in enumerate(chunks):
            m = None if masked else m_buf[:, rng]
            for slot in slots:
                s = dot_nn(kv_s[slot, KEY], q_t[:, rng])
                if masked:
                    key = lax.broadcasted_iota(jnp.int32, s.shape, 0)
                    tok = lax.broadcasted_iota(jnp.int32, s.shape, 1) // n_grp + (c * CHUNK // n_grp) + core * c_len
                    s = jnp.where(tok >= key, s, NEG_BIG)
                s_buf[slot, :, rng] = s
                top = jnp.max(fold(s), axis=0)
                m = top if m is None else jnp.maximum(m, top)
                if with_dp:
                    dp_buf[slot, :, rng] = dot_nn(kv_s[slot, VALUE], do_t[:, rng])
            m_buf[:, rng] = m

    def value_step(slots):
        for rng in chunks:
            l = l_buf[:, rng]
            acc = acc_buf[:, rng]
            for slot in slots:
                w = jnp.exp2(fold(s_buf[slot, :, rng]) * to_log2 - top_buf[:, rng])
                l = l + jnp.sum(w, axis=0)
                acc = acc + dot_tn(kv_s[slot, VALUE], w.reshape(width, CHUNK).astype(BF16))
            l_buf[:, rng] = l
            acc_buf[:, rng] = acc

    def top_step(again):
        for rng in chunks:
            top = spread(jnp.max(m_buf[:, rng], axis=0, keepdims=True) * to_log2)
            if again:
                shrink = jnp.exp2(top_buf[:, rng] - top)
                l_buf[:, rng] = l_buf[:, rng] * shrink
                acc_buf[:, rng] = (fold(acc_buf[:, rng]) * shrink).reshape(d_head, CHUNK)
            top_buf[:, rng] = top

    def pair_loop(first, last, body):
        @pl.loop(0, (last - first) // 2)
        def _(i):
            a, b = first + 2 * i, first + 2 * i + 1
            both = jnp.logical_and(active(a), active(b))
            pl.when(both)(lambda: body([a, b]))
            for slot in (a, b):
                pl.when(jnp.logical_and(active(slot), jnp.logical_not(both)))(functools.partial(body, [slot]))

        if (last - first) % 2:
            pl.when(active(last - 1))(lambda: body([last - 1]))

    def score_body(with_dp, slots):
        for slot in slots:
            cross_copy(slot).wait_recv()
        score_step(slots, False, with_dp)

    def value_body(slots):
        value_step(slots)
        for slot in slots:
            cross_copy(slot).wait_send()

    def score_loop(first, last):
        pair_loop(first, last, functools.partial(score_body, first < n_near))

    def value_loop(first, last):
        pair_loop(first, last, value_body)

    loads[0].wait()
    loads[1].wait()
    arrive(0, 1)
    loads[2].wait()
    loads[3].wait()
    with jax.named_scope("first"):
        q_t[...] = q_s[...].astype(F32).T.astype(BF16)
        do_t[...] = do_s[...].astype(F32).T.astype(BF16)
        l_buf[...] = jnp.zeros(l_buf.shape, F32)
        acc_buf[...] = jnp.zeros(acc_buf.shape, F32)
        cross_copy(0).wait_recv()
        score_step([0], True, True)

    n_next = tree.bounds[2]
    for first, last in ((1, n_next), (n_next, n_near)):
        with jax.named_scope(f"arrive#s={first}"):
            arrive(first, last)
        with jax.named_scope(f"score#s={first}"):
            score_loop(first, last)
    with jax.named_scope("value_near"):
        top_step(False)
        value_loop(0, n_near)
    with jax.named_scope("arrive_far"):
        arrive(n_near, n_slot)
    with jax.named_scope("score_far"):
        score_loop(n_near, n_slot)
    with jax.named_scope("value_far"):
        top_step(True)
        value_loop(n_near, n_slot)

    with jax.named_scope("out"):
        for rng in chunks:
            l = spread(jnp.sum(l_buf[:, rng], axis=0, keepdims=True))
            out = (fold(acc_buf[:, rng]) / l).reshape(d_head, CHUNK).astype(BF16).astype(F32)
            o_out[rng, :] = out.T.astype(BF16)
            top_buf[:, rng] = top_buf[:, rng] + jnp.log2(l)
            d_buf[:, rng] = spread(jnp.sum(do_t[:, rng].astype(F32) * out, axis=0, keepdims=True))
        acc_buf[...] = jnp.zeros(acc_buf.shape, F32)
        for slot in range(n_near):
            each_target(slot, lambda *which: gather_copy(*which).wait_send())

    def grad_step(slot):
        for rng in chunks:
            p = jnp.exp2(fold(s_buf[slot, :, rng]) * to_log2 - top_buf[:, rng])
            dp = dp_buf[slot, :, rng] if slot < n_near else dot_nn(kv_s[slot, VALUE], do_t[:, rng])
            ds = p * (fold(dp) - d_buf[:, rng])
            p_buf[:, rng] = p.reshape(width, CHUNK).astype(BF16)
            ds_buf[slot, :, rng] = ds.reshape(width, CHUNK).astype(BF16)
        for h in range(2):
            keys = pl.ds(h * c_len, c_len)
            part[slot, h, KEY] = dot_nn(ds_buf[slot, keys, :], q_s[...])
            part[slot, h, VALUE] = dot_nn(p_buf[keys, :], do_s[...])

    def zero_step(slot):
        part[slot] = jnp.zeros(part.shape[1:], F32)

    def merge(slot):
        @pl.when(active(slot))
        def _():
            side_copy(slot).wait_recv()
            part[slot, core] = part[slot, core] + side_in[slot]

        for tensor in (KEY, VALUE):
            for child in tree.children(tensor, tree.order[slot]):
                @pl.when(given(tensor, slot, child))
                def _():
                    tree_copy(tensor, child).wait_recv()
                    part[slot, core, tensor] = part[slot, core, tensor] + tree_in[tensor, child]
            if slot:
                pl.when(concerns(slot, tree.givers(tensor, slot)))(tree_copy(tensor, slot).start)
        if slot == 0:
            dk_out[...] = (part[0, core, KEY] * scale).astype(BF16)
            dv_out[...] = part[0, core, VALUE].astype(BF16)

    def sums_sent(slots):
        for slot in slots:
            for tensor in (KEY, VALUE):
                pl.when(concerns(slot, tree.givers(tensor, slot)))(tree_copy(tensor, slot).wait_send)

    def query_step(slots):
        for rng in chunks:
            acc = acc_buf[:, rng]
            for slot in slots:
                acc = acc + dot_tn(kv_s[slot, KEY], ds_buf[slot, :, rng])
            acc_buf[:, rng] = acc

    def queries(slots):
        for a, b in zip(slots[::2], slots[1::2]):
            both = jnp.logical_and(active(a), active(b))
            pl.when(both)(functools.partial(query_step, [a, b]))
            for slot in (a, b):
                pl.when(jnp.logical_and(active(slot), jnp.logical_not(both)))(functools.partial(query_step, [slot]))
        if len(slots) % 2:
            pl.when(active(slots[-1]))(functools.partial(query_step, [slots[-1]]))

    order = [which for what, which in PLAN if what == GRAD]
    sums = [which for what, which in PLAN if what == SUM]
    asked = 0
    for what, which in PLAN:
        if what == GRAD:
            with jax.named_scope(f"grad#s={which}"):
                pl.when(active(which))(functools.partial(grad_step, which))
                pl.when(jnp.logical_not(active(which)))(functools.partial(zero_step, which))
            pl.when(active(which))(side_copy(which).start)
        elif what == SUM:
            with jax.named_scope(f"merge#s={which}"):
                merge(which)
        else:
            with jax.named_scope(f"query#n={which}"):
                queries(order[asked:asked + which])
            asked += which

    with jax.named_scope("query"):
        queries(order[asked:])
        for rng in chunks:
            dq_out[rng, :] = (acc_buf[:, rng] * scale).T.astype(BF16)
    with jax.named_scope("drain"):
        sums_sent(sums[:-4])

        @pl.loop(0, n_slot)
        def _(slot):
            pl.when(active(slot))(lambda: side_copy(slot).wait_send())

    with jax.named_scope("merge#s=0"):
        merge(0)
    sums_sent(sums[-4:])


def store_kernel(*refs):
    *pairs, sem = refs
    half = len(pairs) // 2
    copies = [pltpu.make_async_copy(src, dst, sem.at[i]) for i, (src, dst) in enumerate(zip(pairs[:half], pairs[half:]))]
    for copy in copies:
        copy.start()
    for copy in copies:
        copy.wait()


def solution(mesh):
    part_spec = P("dp", "ctx")
    n_dev = mesh.shape["ctx"]
    tree = Tree(math.isqrt(n_dev // 2))

    def local_step(queries, keys, values, grad_out):
        n_batch, c_len, n_q, d_head = queries.shape
        n_kv = keys.shape[2]
        n_grp = n_q // n_kv
        rows = c_len * n_q
        width = 2 * c_len
        n_slot = n_dev // 2
        scale = d_head ** -0.5
        any_spec = pl.BlockSpec(memory_space=pl.ANY)
        dma_sem = pltpu.SemaphoreType.DMA
        shapes = [(rows, d_head)] * 2 + [(c_len, d_head)] * 2
        results = pl.pallas_call(
            functools.partial(attn_kernel, tree, n_grp, scale),
            out_shape=[pltpu.VMEM(shape, BF16) for shape in shapes],
            in_specs=[any_spec] * 4,
            out_specs=[pl.BlockSpec(memory_space=pltpu.VMEM)] * 4,
            scratch_shapes=[
                pltpu.VMEM((rows, d_head), BF16),
                pltpu.VMEM((rows, d_head), BF16),
                pltpu.VMEM((n_slot, 2, width, d_head), BF16),
                pltpu.VMEM((d_head, rows), BF16),
                pltpu.VMEM((d_head, rows), BF16),
                pltpu.VMEM((n_slot, width, rows), F32),
                pltpu.VMEM((tree.n_near, width, rows), F32),
                pltpu.VMEM((n_slot, width, rows), BF16),
                pltpu.VMEM((width, rows), BF16),
                pltpu.VMEM((SUBLANES, rows), F32),
                pltpu.VMEM((SUBLANES, rows), F32),
                pltpu.VMEM((SUBLANES, rows), F32),
                pltpu.VMEM((d_head, rows), F32),
                pltpu.VMEM((SUBLANES, rows), F32),
                pltpu.VMEM((n_slot, 2, 2, c_len, d_head), F32),
                pltpu.VMEM((n_slot, 2, c_len, d_head), F32),
                pltpu.VMEM((2, n_slot, c_len, d_head), F32),
                dma_sem((4,)),
                dma_sem((n_slot,)),
                dma_sem((n_slot,)),
                dma_sem((n_slot,)),
                dma_sem((2, n_slot)),
                dma_sem((2, n_slot)),
            ],
            compiler_params=pltpu.CompilerParams(
                vmem_limit_bytes=60 * 1024 * 1024, collective_id=0, has_side_effects=True),
            name="attn",
        )(queries.reshape(rows, d_head), grad_out.reshape(rows, d_head),
          keys.reshape(c_len, d_head), values.reshape(c_len, d_head))
        out, dq, dk, dv = pl.pallas_call(
            store_kernel,
            out_shape=[jax.ShapeDtypeStruct(shape, BF16) for shape in shapes],
            in_specs=[pl.BlockSpec(memory_space=pltpu.VMEM)] * 4,
            out_specs=[any_spec] * 4,
            scratch_shapes=[dma_sem((4,))],
            compiler_params=pltpu.CompilerParams(vmem_limit_bytes=2 * 1024 * 1024),
            name="store",
        )(*results)
        q_shape = (n_batch, c_len, n_q, d_head)
        kv_shape = (n_batch, c_len, n_kv, d_head)
        return out.reshape(q_shape), dq.reshape(q_shape), dk.reshape(kv_shape), dv.reshape(kv_shape)

    return jax.shard_map(local_step, mesh=mesh, in_specs=(part_spec,) * 4, out_specs=(part_spec,) * 4, check_vma=False)
```

```python
import functools
import math

import jax
import jax.numpy as jnp
from jax import lax
from jax.experimental import pallas as pl
from jax.experimental.pallas import tpu as pltpu
from jax.sharding import PartitionSpec as P

NEG_BIG = -1e30
CHUNK = 256
SUBLANES = 8
KEY, VALUE = 0, 1
F32 = jnp.float32
BF16 = jnp.bfloat16
GRAD, SUM, QUERY = 0, 1, 2
PLAN = (
    (GRAD, 15), (GRAD, 11), (GRAD, 12), (SUM, 15), (GRAD, 13), (SUM, 11), (GRAD, 7), (SUM, 12), (GRAD, 14),
    (SUM, 13), (GRAD, 9), (GRAD, 1), (SUM, 7), (SUM, 14), (GRAD, 10), (SUM, 9), (QUERY, 2), (SUM, 1), (QUERY, 2),
    (QUERY, 2), (QUERY, 2), (SUM, 10), (GRAD, 5), (GRAD, 4), (GRAD, 8), (GRAD, 6), (QUERY, 2), (SUM, 5), (SUM, 8),
    (QUERY, 2), (GRAD, 3), (SUM, 6), (GRAD, 2), (SUM, 4), (GRAD, 0), (SUM, 2), (SUM, 3), (QUERY, 2), (QUERY, 2),
)
PARENTS = (
    (None, (0, 1), (0, 3), (1, 0), (3, 0), (1, 1), (0, 3), (0, 1), (3, 0), (0, 3), (1, 0), (0, 1), (1, 0), (3, 0), (3, 3), (1, 1)),
    (None, (0, 1), (0, 3), (1, 0), (3, 0), (1, 1), (1, 3), (0, 1), (3, 0), (0, 3), (3, 0), (0, 3), (1, 0), (1, 0), (3, 3), (3, 3)),
)


def dot_tn(a, b):
    return lax.dot_general(a, b, (((0,), (0,)), ((), ())), preferred_element_type=F32)


def dot_nn(a, b):
    return jnp.dot(a, b, preferred_element_type=F32)


def fold(x):
    return x.reshape(x.shape[0] // SUBLANES, SUBLANES, x.shape[1])


def spread(x):
    return jnp.broadcast_to(x, (SUBLANES, x.shape[1]))


class Tree:
    def __init__(self, side):
        self.side = side
        offsets = [(dx, dy) for dx in range(side) for dy in range(side)]
        mid = side // 2

        def group(o):
            if mid in o:
                return 3 if 0 in o else 5 if o == (mid, mid) else 4
            return 0 if o == (0, 0) else 1 if 0 in o else 2

        self.order = sorted(offsets, key=lambda o: (group(o), o))
        kinds = [group(o) for o in self.order]
        self.bounds = [kinds.index(k) for k in range(5)] + [len(kinds)]
        self.n_near = self.bounds[3]
        self.slot = {o: i for i, o in enumerate(self.order)}

    def parent(self, tensor, off):
        return PARENTS[tensor][self.slot[off]]

    def children(self, tensor, off):
        return [there for there in range(1, len(self.order)) if off == tuple(
            (o - p) % self.side for o, p in zip(self.order[there], self.parent(tensor, self.order[there])))]

    def source(self, off):
        side = self.side
        mid, one, far = side // 2, 1, side - 1
        if mid not in off:
            return off
        if off == (mid, mid):
            return (one, one)
        if off[0] == mid:
            return (one if off[1] == 0 else far, 0)
        return (0, one if off[0] == 0 else far)

    def targets(self, slot):
        found = []
        for there in range(1, len(self.order)):
            src = self.source(self.order[there])
            if tuple((o - e) % self.side for o, e in zip(self.order[there], src)) == self.order[slot]:
                found.append((tuple((-e) % self.side for e in src), there))
        return found


    def takers(self, slot):
        found = [(0, 0)]
        for off, there in self.targets(slot):
            found += [self.move(off, o) for o in self.takers(there)]
        return found

    def givers(self, tensor, slot):
        found = [(0, 0)]
        for child in self.children(tensor, self.order[slot]):
            hop = self.hop_to(slot, child)
            found += [self.move(hop, o) for o in self.givers(tensor, child)]
        return found

    def move(self, a, b):
        return tuple((i + j) % self.side for i, j in zip(a, b))

    def hop_to(self, slot, child):
        return tuple((i - j) % self.side for i, j in zip(self.order[slot], self.order[child]))


def attn_kernel(tree, n_grp, scale, q_hbm, do_hbm, k_hbm, v_hbm, o_out, dq_out, dk_out, dv_out,
                q_s, do_s, kv_s, q_t, do_t, s_buf, dp_buf, ds_buf, p_buf, m_buf, top_buf, l_buf, acc_buf, d_buf,
                part, side_in, tree_in, local_sem, gather_sem, cross_sem, side_sem, tree_sem, sent_sem):
    rows, d_head = q_s.shape
    c_len = k_hbm.shape[0]
    width = 2 * c_len
    side = tree.side
    n_slot = side * side
    n_near = tree.n_near
    dev = lax.axis_index("ctx")
    core = lax.rem(dev, 2)
    mine = dev // 2
    at_x = lax.rem(mine, side)
    at_y = mine // side
    sibling = {"ctx": mine * 2 + 1 - core}
    chunks = [pl.ds(i * CHUNK, CHUNK) for i in range(rows // CHUNK)]
    to_log2 = scale * math.log2(math.e)
    own_rows = pl.ds(pl.multiple_of(core * c_len, c_len), c_len)

    def chip_at(off):
        return lax.rem(at_y + off[1], side) * side + lax.rem(at_x + off[0], side)

    def near(off):
        return {"ctx": chip_at(off) * 2 + core}

    loads = [
        pltpu.make_async_copy(k_hbm, kv_s.at[0, KEY, own_rows, :], local_sem.at[0]),
        pltpu.make_async_copy(v_hbm, kv_s.at[0, VALUE, own_rows, :], local_sem.at[1]),
        pltpu.make_async_copy(q_hbm, q_s, local_sem.at[2]),
        pltpu.make_async_copy(do_hbm, do_s, local_sem.at[3]),
    ]
    for copy in loads:
        copy.start()

    with jax.named_scope("barrier"):
        barrier = pltpu.get_barrier_semaphore()
        peers = [near(off) for off in tree.order[1:n_near]] + [sibling]
        for peer in peers:
            pl.semaphore_signal(barrier, inc=1, device_id=peer, device_id_type=pl.DeviceIdType.MESH)
        pl.semaphore_wait(barrier, len(peers))

    def remote(src, dst, send, recv, peer):
        return pltpu.make_async_remote_copy(src_ref=src, dst_ref=dst, send_sem=send, recv_sem=recv,
                                            device_id=peer, device_id_type=pl.DeviceIdType.MESH)

    def gather_copy(slot, off, there):
        return remote(kv_s.at[slot, :, own_rows, :], kv_s.at[there, :, own_rows, :],
                      sent_sem.at[0, there], gather_sem.at[there], near(off))

    def cross_copy(slot):
        block = kv_s.at[slot, :, own_rows, :]
        return remote(block, block, sent_sem.at[1, slot], cross_sem.at[slot], sibling)

    def side_copy(slot):
        return remote(part.at[slot, 1 - core], side_in.at[slot], sent_sem.at[1, slot], side_sem.at[slot], sibling)

    def tree_copy(tensor, slot):
        hop = tree.parent(tensor, tree.order[slot])
        return remote(part.at[slot, core, tensor], tree_in.at[tensor, slot],
                      (gather_sem, cross_sem)[tensor].at[slot], tree_sem.at[tensor, slot], near(hop))

    def concerns(slot, offsets):
        owner = chip_at(tree.order[slot])
        return functools.reduce(jnp.logical_or, [chip_at(o) >= owner for o in offsets])

    def taken(slot, off, there):
        return concerns(slot, [tree.move(off, o) for o in tree.takers(there)])

    def given(tensor, slot, child):
        return concerns(slot, [tree.move(tree.hop_to(slot, child), o) for o in tree.givers(tensor, child)])

    def active(slot):
        owner = chip_at(tree.order[slot]) if isinstance(slot, int) else slot_chip(slot)
        return owner <= mine

    def each_target(slot, act):
        for off, there in tree.targets(slot):
            pl.when(taken(slot, off, there))(functools.partial(act, slot, off, there))

    def arrive(first, last):
        for slot in range(first, last):
            if slot:
                pl.when(concerns(slot, tree.takers(slot)))(
                    gather_copy(slot, tree.source(tree.order[slot]), slot).wait_recv)
            each_target(slot, lambda *which: gather_copy(*which).start())
            pl.when(active(slot))(cross_copy(slot).start)

    xs = sum(o[0] << (2 * i) for i, o in enumerate(tree.order))
    ys = sum(o[1] << (2 * i) for i, o in enumerate(tree.order))

    def slot_chip(slot):
        def field(packed):
            signed = packed - (1 << 32) if packed >= 1 << 31 else packed
            return lax.shift_right_logical(jnp.int32(signed), 2 * slot) & 3
        return chip_at((field(xs), field(ys)))

    def score_step(slots, masked, with_dp):
        for c, rng in enumerate(chunks):
            m = None if masked else m_buf[:, rng]
            for slot in slots:
                s = dot_nn(kv_s[slot, KEY], q_t[:, rng])
                if masked:
                    key = lax.broadcasted_iota(jnp.int32, s.shape, 0)
                    tok = lax.broadcasted_iota(jnp.int32, s.shape, 1) // n_grp + (c * CHUNK // n_grp) + core * c_len
                    s = jnp.where(tok >= key, s, NEG_BIG)
                s_buf[slot, :, rng] = s
                top = jnp.max(fold(s), axis=0)
                m = top if m is None else jnp.maximum(m, top)
                if with_dp:
                    dp_buf[slot, :, rng] = dot_nn(kv_s[slot, VALUE], do_t[:, rng])
            m_buf[:, rng] = m

    def value_step(slots):
        for rng in chunks:
            l = l_buf[:, rng]
            acc = acc_buf[:, rng]
            for slot in slots:
                w = jnp.exp2(fold(s_buf[slot, :, rng]) * to_log2 - top_buf[:, rng])
                l = l + jnp.sum(w, axis=0)
                acc = acc + dot_tn(kv_s[slot, VALUE], w.reshape(width, CHUNK).astype(BF16))
            l_buf[:, rng] = l
            acc_buf[:, rng] = acc

    def top_step(again):
        for rng in chunks:
            top = spread(jnp.max(m_buf[:, rng], axis=0, keepdims=True) * to_log2)
            if again:
                shrink = jnp.exp2(top_buf[:, rng] - top)
                l_buf[:, rng] = l_buf[:, rng] * shrink
                acc_buf[:, rng] = (fold(acc_buf[:, rng]) * shrink).reshape(d_head, CHUNK)
            top_buf[:, rng] = top

    def pair_loop(first, last, body):
        @pl.loop(0, (last - first) // 2)
        def _(i):
            a, b = first + 2 * i, first + 2 * i + 1
            both = jnp.logical_and(active(a), active(b))
            pl.when(both)(lambda: body([a, b]))
            for slot in (a, b):
                pl.when(jnp.logical_and(active(slot), jnp.logical_not(both)))(functools.partial(body, [slot]))

        if (last - first) % 2:
            pl.when(active(last - 1))(lambda: body([last - 1]))

    def score_body(with_dp, slots):
        for slot in slots:
            cross_copy(slot).wait_recv()
        score_step(slots, False, with_dp)

    def value_body(slots):
        value_step(slots)
        for slot in slots:
            cross_copy(slot).wait_send()

    def score_loop(first, last):
        pair_loop(first, last, functools.partial(score_body, first < n_near))

    def value_loop(first, last):
        pair_loop(first, last, value_body)

    loads[0].wait()
    loads[1].wait()
    arrive(0, 1)
    loads[2].wait()
    loads[3].wait()
    with jax.named_scope("first"):
        q_t[...] = q_s[...].astype(F32).T.astype(BF16)
        do_t[...] = do_s[...].astype(F32).T.astype(BF16)
        l_buf[...] = jnp.zeros(l_buf.shape, F32)
        acc_buf[...] = jnp.zeros(acc_buf.shape, F32)
        cross_copy(0).wait_recv()
        score_step([0], True, True)

    n_next = tree.bounds[2]
    for first, last in ((1, n_next), (n_next, n_near)):
        with jax.named_scope(f"arrive#s={first}"):
            arrive(first, last)
        with jax.named_scope(f"score#s={first}"):
            score_loop(first, last)
    with jax.named_scope("value_near"):
        top_step(False)
        value_loop(0, n_near)
    with jax.named_scope("arrive_far"):
        arrive(n_near, n_slot)
    with jax.named_scope("score_far"):
        score_loop(n_near, n_slot)
    with jax.named_scope("value_far"):
        top_step(True)
        value_loop(n_near, n_slot)

    with jax.named_scope("out"):
        for rng in chunks:
            l = spread(jnp.sum(l_buf[:, rng], axis=0, keepdims=True))
            out = (fold(acc_buf[:, rng]) / l).reshape(d_head, CHUNK).astype(BF16).astype(F32)
            o_out[rng, :] = out.T.astype(BF16)
            top_buf[:, rng] = top_buf[:, rng] + jnp.log2(l)
            d_buf[:, rng] = spread(jnp.sum(do_t[:, rng].astype(F32) * out, axis=0, keepdims=True))
        acc_buf[...] = jnp.zeros(acc_buf.shape, F32)
        for slot in range(n_near):
            each_target(slot, lambda *which: gather_copy(*which).wait_send())

    def grad_step(slot):
        for rng in chunks:
            p = jnp.exp2(fold(s_buf[slot, :, rng]) * to_log2 - top_buf[:, rng])
            dp = dp_buf[slot, :, rng] if slot < n_near else dot_nn(kv_s[slot, VALUE], do_t[:, rng])
            ds = p * (fold(dp) - d_buf[:, rng])
            p_buf[:, rng] = p.reshape(width, CHUNK).astype(BF16)
            ds_buf[slot, :, rng] = ds.reshape(width, CHUNK).astype(BF16)
        for h in range(2):
            keys = pl.ds(h * c_len, c_len)
            part[slot, h, KEY] = dot_nn(ds_buf[slot, keys, :], q_s[...])
            part[slot, h, VALUE] = dot_nn(p_buf[keys, :], do_s[...])

    def zero_step(slot):
        part[slot] = jnp.zeros(part.shape[1:], F32)

    def merge(slot):
        @pl.when(active(slot))
        def _():
            side_copy(slot).wait_recv()
            part[slot, core] = part[slot, core] + side_in[slot]

        for tensor in (KEY, VALUE):
            for child in tree.children(tensor, tree.order[slot]):
                @pl.when(given(tensor, slot, child))
                def _():
                    tree_copy(tensor, child).wait_recv()
                    part[slot, core, tensor] = part[slot, core, tensor] + tree_in[tensor, child]
            if slot:
                pl.when(concerns(slot, tree.givers(tensor, slot)))(tree_copy(tensor, slot).start)
        if slot == 0:
            dk_out[...] = (part[0, core, KEY] * scale).astype(BF16)
            dv_out[...] = part[0, core, VALUE].astype(BF16)

    def sums_sent(slots):
        for slot in slots:
            for tensor in (KEY, VALUE):
                pl.when(concerns(slot, tree.givers(tensor, slot)))(tree_copy(tensor, slot).wait_send)

    def query_step(slots):
        for rng in chunks:
            acc = acc_buf[:, rng]
            for slot in slots:
                acc = acc + dot_tn(kv_s[slot, KEY], ds_buf[slot, :, rng])
            acc_buf[:, rng] = acc

    def queries(slots):
        for a, b in zip(slots[::2], slots[1::2]):
            both = jnp.logical_and(active(a), active(b))
            pl.when(both)(functools.partial(query_step, [a, b]))
            for slot in (a, b):
                pl.when(jnp.logical_and(active(slot), jnp.logical_not(both)))(functools.partial(query_step, [slot]))
        if len(slots) % 2:
            pl.when(active(slots[-1]))(functools.partial(query_step, [slots[-1]]))

    order = [which for what, which in PLAN if what == GRAD]
    sums = [which for what, which in PLAN if what == SUM]
    asked = 0
    for what, which in PLAN:
        if what == GRAD:
            with jax.named_scope(f"grad#s={which}"):
                pl.when(active(which))(functools.partial(grad_step, which))
                pl.when(jnp.logical_not(active(which)))(functools.partial(zero_step, which))
            pl.when(active(which))(side_copy(which).start)
        elif what == SUM:
            with jax.named_scope(f"merge#s={which}"):
                merge(which)
        else:
            with jax.named_scope(f"query#n={which}"):
                queries(order[asked:asked + which])
            asked += which

    with jax.named_scope("query"):
        queries(order[asked:])
        for rng in chunks:
            dq_out[rng, :] = (acc_buf[:, rng] * scale).T.astype(BF16)
    with jax.named_scope("drain"):
        sums_sent(sums[:-4])

        @pl.loop(0, n_slot)
        def _(slot):
            pl.when(active(slot))(lambda: side_copy(slot).wait_send())

    with jax.named_scope("merge#s=0"):
        merge(0)
    sums_sent(sums[-4:])


def store_kernel(*refs):
    *pairs, sem = refs
    half = len(pairs) // 2
    copies = [pltpu.make_async_copy(src, dst, sem.at[i]) for i, (src, dst) in enumerate(zip(pairs[:half], pairs[half:]))]
    for copy in copies:
        copy.start()
    for copy in copies:
        copy.wait()


def solution(mesh):
    part_spec = P("dp", "ctx")
    n_dev = mesh.shape["ctx"]
    tree = Tree(math.isqrt(n_dev // 2))

    def local_step(queries, keys, values, grad_out):
        n_batch, c_len, n_q, d_head = queries.shape
        n_kv = keys.shape[2]
        n_grp = n_q // n_kv
        rows = c_len * n_q
        width = 2 * c_len
        n_slot = n_dev // 2
        scale = d_head ** -0.5
        any_spec = pl.BlockSpec(memory_space=pl.ANY)
        dma_sem = pltpu.SemaphoreType.DMA
        shapes = [(rows, d_head)] * 2 + [(c_len, d_head)] * 2
        results = pl.pallas_call(
            functools.partial(attn_kernel, tree, n_grp, scale),
            out_shape=[pltpu.VMEM(shape, BF16) for shape in shapes],
            in_specs=[any_spec] * 4,
            out_specs=[pl.BlockSpec(memory_space=pltpu.VMEM)] * 4,
            scratch_shapes=[
                pltpu.VMEM((rows, d_head), BF16),
                pltpu.VMEM((rows, d_head), BF16),
                pltpu.VMEM((n_slot, 2, width, d_head), BF16),
                pltpu.VMEM((d_head, rows), BF16),
                pltpu.VMEM((d_head, rows), BF16),
                pltpu.VMEM((n_slot, width, rows), F32),
                pltpu.VMEM((tree.n_near, width, rows), F32),
                pltpu.VMEM((n_slot, width, rows), BF16),
                pltpu.VMEM((width, rows), BF16),
                pltpu.VMEM((SUBLANES, rows), F32),
                pltpu.VMEM((SUBLANES, rows), F32),
                pltpu.VMEM((SUBLANES, rows), F32),
                pltpu.VMEM((d_head, rows), F32),
                pltpu.VMEM((SUBLANES, rows), F32),
                pltpu.VMEM((n_slot, 2, 2, c_len, d_head), F32),
                pltpu.VMEM((n_slot, 2, c_len, d_head), F32),
                pltpu.VMEM((2, n_slot, c_len, d_head), F32),
                dma_sem((4,)),
                dma_sem((n_slot,)),
                dma_sem((n_slot,)),
                dma_sem((n_slot,)),
                dma_sem((2, n_slot)),
                dma_sem((2, n_slot)),
            ],
            compiler_params=pltpu.CompilerParams(
                vmem_limit_bytes=60 * 1024 * 1024, collective_id=0, has_side_effects=True),
            name="attn",
        )(queries.reshape(rows, d_head), grad_out.reshape(rows, d_head),
          keys.reshape(c_len, d_head), values.reshape(c_len, d_head))
        out, dq, dk, dv = pl.pallas_call(
            store_kernel,
            out_shape=[jax.ShapeDtypeStruct(shape, BF16) for shape in shapes],
            in_specs=[pl.BlockSpec(memory_space=pltpu.VMEM)] * 4,
            out_specs=[any_spec] * 4,
            scratch_shapes=[dma_sem((4,))],
            compiler_params=pltpu.CompilerParams(vmem_limit_bytes=2 * 1024 * 1024),
            name="store",
        )(*results)
        q_shape = (n_batch, c_len, n_q, d_head)
        kv_shape = (n_batch, c_len, n_kv, d_head)
        return out.reshape(q_shape), dq.reshape(q_shape), dk.reshape(kv_shape), dv.reshape(kv_shape)

    return jax.shard_map(local_step, mesh=mesh, in_specs=(part_spec,) * 4, out_specs=(part_spec,) * 4, check_vma=False)
```
